128 devices in a mesh: walk: 8 (over y, x_lo), orb: 16 (over x_hi, z, core).
Axes of the slice: x: 4 (x_hi: 2, x_lo: 2; x = x_hi * 2 + x_lo), y: 4, z: 4, core: 2. Of those that a mesh axis runs over, the one named last changes fastest.
Arguments:
- coefficients: bfloat16 [4096, 4096], P(None, 'orb'), may hold values from -6 to 6
- inverse: bfloat16 [8, 1024, 1024], P('walk', 'orb'), may hold values from -0.005859375 to 0.005859375
- cell_index: int32 [8, 3, 1024], P('walk'), may hold values from 0 to 15
- fraction: float32 [8, 3, 1024], P('walk'), may hold values from 0 to 1
- energies: float32 [8], P('walk'), may hold values from -8 to 8
- weights: float32 [8], P('walk'), may hold values from 0.5 to 2
- occupied: int32 [1024], replicated, may hold values from 0 to 4095, as said below
Outputs:
- gradient: float32 [1024, 4096], P('walk', 'orb')
The draws below stay inside these ranges and needn't reach their ends.
Inputs may be any that keep to these rules, and one draw needn't show every extreme that they name: `occupied`: 1024 distinct orbital indices; every block of 256 consecutive orbital indices holds at most 96 of them, and some block holds exactly 96.
All inputs are finite; a program needn't handle non-finite values.
Results may differ from the reference program's by a relative error of at most 0.019.
Values may be sent and summed in bfloat16 or wider, within the bound.
No kernel may reach another device: no remote copies, remote signals or barrier semaphores. Data moves between devices by JAX's collectives and lax.ppermute only.
A program may use at most 64 MiB of HBM per device.

```python
import math
import jax
import jax.numpy as jnp
from jax import lax

N = 1024
M = 4096
GRID = 16
SAMPLES = 8
CELLS = 4096
N_ORB = 16


def draw_occupied(key, part):
    shards = N_ORB
    local = M // N_ORB
    bound = 3 * N // (2 * N_ORB)
    others = shards - 1
    remainder = N - bound
    base = remainder // others
    extra = remainder - base * others
    key_moves = jax.random.fold_in(key, 11)
    key_spot = jax.random.fold_in(key, 12)
    key_score = jax.random.fold_in(key, 13)
    key_order = jax.random.fold_in(key, 14)
    counts = base + (jnp.arange(others, dtype=jnp.int32) < extra).astype(jnp.int32)
    margin = max(0, min(base - 1, bound - base - 2))
    pairs = others // 2
    moves = jax.random.randint(key_moves, (pairs,), 0, margin + 1).astype(jnp.int32)
    change = jnp.zeros((others,), jnp.int32)
    change = change.at[0:2 * pairs:2].add(moves)
    change = change.at[1:2 * pairs:2].add(-moves)
    counts = counts + change
    full = jnp.concatenate([jnp.full((1,), bound, jnp.int32), counts])
    spot = jax.random.randint(key_spot, (), 0, shards)
    full = jnp.roll(full, spot)
    scores = jax.random.randint(key_score, (shards, local), 0, 1 << 20).astype(jnp.int32) * local + jnp.arange(local, dtype=jnp.int32)[None, :]
    scores = scores.at[0, 0].set(-1)
    scores = scores.at[shards - 1, local - 1].set(-1)
    ranking = jnp.argsort(jnp.argsort(scores, axis=1), axis=1).astype(jnp.int32)
    chosen = (ranking < full[:, None]).reshape(-1)
    orbital_ids = jnp.arange(shards * local, dtype=jnp.int32)
    keyed = jnp.where(chosen, orbital_ids, orbital_ids + shards * local)
    picked = jnp.sort(keyed)[:N]
    return jax.random.permutation(key_order, picked).astype(jnp.int32)


def with_ends(array, key, low, top_value):
    spot = [jax.random.randint(jax.random.fold_in(key, axis), (), 0, length) for axis, length in enumerate(array.shape)]
    main_axis = array.shape.index(max(array.shape))
    neighbour = spot[:main_axis] + [(spot[main_axis] + 1) % array.shape[main_axis]] + spot[main_axis + 1:]
    return array.at[tuple(spot)].set(low).at[tuple(neighbour)].set(top_value)


def block_levels(stream_key, dims, pieces, low, top_value):
    gain = 1.0
    for axis_at, shards_of in pieces:
        steps = jax.random.uniform(jax.random.fold_in(jax.random.fold_in(stream_key, 6), axis_at), (shards_of,), jnp.float32, low / len(pieces), top_value / len(pieces))
        gain = gain * jnp.repeat(jnp.exp(steps), dims[axis_at] // shards_of).reshape((-1,) + (1,) * (len(dims) - 1 - axis_at))
    return gain


def gaussian(stream_key, shape, deviation, most, cuts=(), held_as=jnp.bfloat16):
    result = jax.random.normal(stream_key, shape, jnp.float32) * deviation
    if len(cuts) > 0:
        result = block_levels(stream_key, shape, cuts, -0.22, 0.18) * result
    return jnp.clip(result, min=-most, max=most).astype(held_as)


def setup_inputs(seed: int = 0) -> dict:
    seeds = jax.random.split(jax.random.key(seed), 8)
    coefficients = gaussian(seeds[0], (CELLS, M), 1.0, 6.0, ((1, 16),))
    inverse = gaussian(seeds[1], (SAMPLES, N, N), (N * N) ** -0.5, 0.005859375, ((0, 8), (1, 16)))
    cell_index = with_ends(jax.random.randint(seeds[2], (SAMPLES, 3, N), 0, GRID), jax.random.fold_in(seeds[2], 1), 0, GRID - 1).astype(jnp.int32)
    fraction = jnp.clip(1.0 * jax.random.uniform(seeds[3], (SAMPLES, 3, N), jnp.float32) ** block_levels(seeds[3], (SAMPLES, 3, N), ((0, 8),), -0.2, 0.2), 0.0, 1.0)
    energies = gaussian(seeds[4], (SAMPLES,), 2.0, 8.0, ((0, 8),), jnp.float32)
    weights = jnp.clip(jnp.exp(math.log(2.0) - 1.3862944 * jax.random.uniform(seeds[5], (SAMPLES,), jnp.float32) ** block_levels(seeds[5], (SAMPLES,), ((0, 8),), -0.2, 0.2)), 0.5, 2.0)
    occupied = draw_occupied(jax.random.fold_in(seeds[7], 71), 0)
    return dict(coefficients=coefficients, inverse=inverse, cell_index=cell_index, fraction=fraction, energies=energies, weights=weights, occupied=occupied)


def spline_basis(frac):
    remain = 1.0 - frac
    square = frac * frac
    cubed = square * frac
    values = jnp.stack([remain * remain * remain, 3.0 * cubed - 6.0 * square + 4.0, -3.0 * cubed + 3.0 * square + 3.0 * frac + 1.0, cubed]) / 6.0
    curves = jnp.stack([remain, 3.0 * frac - 2.0, 1.0 - 3.0 * frac, frac])
    return values, curves


def evaluate(coefficients, cell_one, frac_one, edge):
    shifts = jnp.arange(4, dtype=jnp.int32)[:, None] - 1
    index_x = (cell_one[0][None, :] + shifts) % edge
    index_y = (cell_one[1][None, :] + shifts) % edge
    index_z = (cell_one[2][None, :] + shifts) % edge
    value_x, curve_x = spline_basis(frac_one[0])
    value_y, curve_y = spline_basis(frac_one[1])
    value_z, curve_z = spline_basis(frac_one[2])
    plane = (index_y[:, None, :] * edge + index_z[None, :, :]).reshape(16, -1)
    value_yz = (value_y[:, None, :] * value_z[None, :, :]).reshape(16, -1)
    curve_yz = (curve_y[:, None, :] * value_z[None, :, :] + value_y[:, None, :] * curve_z[None, :, :]).reshape(16, -1)
    electrons = cell_one.shape[1]
    orbital_sum = jnp.zeros((electrons, coefficients.shape[1]), jnp.float32)
    laplace_sum = jnp.zeros((electrons, coefficients.shape[1]), jnp.float32)
    for tap_x in range(4):
        tap_rows = index_x[tap_x][None, :] * (edge * edge) + plane
        tap_coef = jnp.take(coefficients, tap_rows, axis=0).astype(jnp.float32)
        weight_val = value_x[tap_x][None, :] * value_yz
        weight_lap = curve_x[tap_x][None, :] * value_yz + value_x[tap_x][None, :] * curve_yz
        orbital_sum = orbital_sum + jnp.einsum("kn,knw->nw", weight_val, tap_coef, precision=lax.Precision.HIGHEST)
        laplace_sum = laplace_sum + jnp.einsum("kn,knw->nw", weight_lap, tap_coef, precision=lax.Precision.HIGHEST)
    return orbital_sum.astype(jnp.bfloat16), laplace_sum.astype(jnp.bfloat16)


def wide_dot(left, right):
    return jnp.dot(left.astype(jnp.float32), right.astype(jnp.float32), precision=lax.Precision.HIGHEST)


def reference(coefficients, inverse, cell_index, fraction, energies, weights, occupied):
    def one_sample(running, items):
        inverse_one, cells_one, frac_one, energy, weight = items
        orbital_vals, laplace_vals = evaluate(coefficients, cells_one, frac_one, GRID)
        ratio = wide_dot(inverse_one, orbital_vals).astype(jnp.bfloat16)
        kinetic = wide_dot(inverse_one, laplace_vals)
        occupied_block = jnp.take(kinetic, occupied, axis=1).astype(jnp.bfloat16)
        coupled = wide_dot(occupied_block, ratio)
        sample_term = weight * (energy * ratio.astype(jnp.float32) - 0.5 * (kinetic - coupled))
        return running + sample_term, None

    initial = jnp.zeros((N, M), jnp.float32)
    gradient, unused = lax.scan(one_sample, initial, (inverse, cell_index, fraction, energies, weights))
    return gradient
```

```python
import functools

import jax
import jax.numpy as jnp
from jax import lax
from jax.experimental import pallas as pl
from jax.experimental.pallas import tpu as pltpu
from jax.sharding import Mesh
from jax.sharding import PartitionSpec as P

GRID = 16
PLANE = GRID * GRID
TILE = 256
BF16 = jnp.bfloat16
F32 = jnp.float32


def mm(left, right):
    return jnp.dot(left, right, preferred_element_type=F32)


def mm_nt(left, right):
    return lax.dot_general(left, right, (((1,), (1,)), ((), ())), preferred_element_type=F32)


def mm_tn(left, right):
    return lax.dot_general(left, right, (((0,), (0,)), ((), ())), preferred_element_type=F32)


def dense_rows(cell, frac):
    remain = 1.0 - frac
    square = frac * frac
    cubed = square * frac
    sixth = 1.0 / 6.0
    values = [
        remain * remain * remain * sixth,
        (3.0 * cubed - 6.0 * square + 4.0) * sixth,
        (-3.0 * cubed + 3.0 * square + 3.0 * frac + 1.0) * sixth,
        cubed * sixth,
    ]
    curves = [remain, 3.0 * frac - 2.0, 1.0 - 3.0 * frac, frac]
    line = lax.broadcasted_iota(jnp.int32, (GRID, cell.shape[1]), 0)
    tap = (line - cell + (GRID + 1)) & (GRID - 1)
    value = jnp.zeros((GRID, cell.shape[1]), F32)
    curve = jnp.zeros((GRID, cell.shape[1]), F32)
    for a in range(4):
        value = jnp.where(tap == a, values[a], value)
        curve = jnp.where(tap == a, curves[a], curve)
    return value, curve


def high_low(x):
    high = x.astype(BF16).astype(F32)
    return [high, x - high]


def eval_kernel(me_ref, coef_ref, cell_ref, frac_ref, occ_ref, val_ref, lap_ref, lapt_ref, slot_ref,
                yz_ref, x_ref, wide_ref, w0_ref, w1_ref, *, shards):
    electrons = cell_ref.shape[1]
    width = coef_ref.shape[1]
    slots = lapt_ref.shape[0]

    me = me_ref[0]
    occ = occ_ref[...]
    owner = lax.broadcasted_iota(jnp.int32, (shards, occ.shape[1]), 0) == lax.div(occ, width)
    count = owner.astype(jnp.int32)
    lane = lax.broadcasted_iota(jnp.int32, count.shape, 1)
    step = 1
    while step < occ.shape[1]:
        count = count + jnp.where(lane >= step, pltpu.roll(count, step, 1), 0)
        step *= 2
    rank = jnp.sum(jnp.where(owner, count - 1, 0), axis=0, keepdims=True)
    slot = lax.div(occ, width) * slots + rank
    slot_ref[...] = slot
    placed = lax.broadcasted_iota(jnp.int32, (slots, occ.shape[1]), 0) == slot - me * slots
    column = lax.broadcasted_iota(jnp.int32, (width, occ.shape[1]), 0) == occ - me * width
    picker = mm_nt(placed.astype(F32).astype(BF16), column.astype(F32).astype(BF16)).astype(BF16)

    vx, cx = dense_rows(cell_ref[0:1, :], frac_ref[0:1, :])
    vy, cy = dense_rows(cell_ref[1:2, :], frac_ref[1:2, :])
    vz, cz = dense_rows(cell_ref[2:3, :], frac_ref[2:3, :])
    table = jnp.concatenate(high_low(vy) + high_low(cy) + high_low(vz) + high_low(cz), axis=0)
    yz_ref[...] = jnp.transpose(table).astype(BF16)
    x_ref[...] = jnp.transpose(jnp.concatenate([vx, cx] * 4, axis=0))

    row = lax.broadcasted_iota(jnp.int32, (8 * GRID, 4 * PLANE), 0)
    col = lax.broadcasted_iota(jnp.int32, (8 * GRID, 4 * PLANE), 1)
    cell_in = col & (PLANE - 1)
    group = row >> 5
    line = jnp.where(group < 2, cell_in >> 4, cell_in & (GRID - 1))
    wide_ref[...] = ((group == (col >> 8)) & (line == (row & (GRID - 1)))).astype(F32).astype(BF16)

    def build(t, w_ref):
        rows = pl.ds(t * TILE, TILE)
        parts = mm(yz_ref[rows, :], wide_ref[...])
        y_value, y_curve = parts[:, :PLANE], parts[:, PLANE:2 * PLANE]
        z_value, z_curve = parts[:, 2 * PLANE:3 * PLANE], parts[:, 3 * PLANE:]
        value = y_value * z_value
        curve = y_curve * z_value + y_value * z_curve
        xs = x_ref[rows, :]
        for g in range(GRID):
            x_value = xs[:, g:g + 1]
            x_curve = xs[:, GRID + g:GRID + g + 1]
            w_ref[:TILE, g * PLANE:(g + 1) * PLANE] = (x_value * value).astype(BF16)
            w_ref[TILE:, g * PLANE:(g + 1) * PLANE] = (x_curve * value + x_value * curve).astype(BF16)

    def product(t, w_ref):
        both = mm(w_ref[...], coef_ref[...]).astype(BF16)
        val_ref[t * TILE:(t + 1) * TILE, :] = both[:TILE]
        lap = both[TILE:]
        lap_ref[t * TILE:(t + 1) * TILE, :] = lap
        lapt_ref[:, t * TILE:(t + 1) * TILE] = mm_nt(picker, lap).astype(BF16)

    slots_w = [w0_ref, w1_ref]
    tiles = electrons // TILE
    build(0, slots_w[0])
    for t in range(tiles):
        if t + 1 < tiles:
            build(t + 1, slots_w[(t + 1) % 2])
        product(t, slots_w[t % 2])


def in_order(out_ref, value, core, size):
    for j in range(value.shape[0] // size):
        start = pl.multiple_of((2 * j + core) * size, size)
        out_ref[pl.ds(start, size), :] = value[j * size:(j + 1) * size].astype(out_ref.dtype)


def ratio_kernel(core_ref, inv_own_ref, inv_other_ref, val_ref, slot_ref, rows_ref, ratio_ref, *, slots, size):
    core = core_ref[0]
    in_order(ratio_ref, mm(inv_own_ref[...], val_ref[...]), core, size)
    in_order(ratio_ref, mm(inv_other_ref[...], val_ref[...]), 1 - core, size)
    ratio = ratio_ref[...]
    slot = slot_ref[...]
    half = rows_ref.shape[0] // 2
    for h in range(2):
        side = core if h == 0 else 1 - core
        for j in range(half // slots):
            ids = lax.broadcasted_iota(jnp.int32, (slots, slot.shape[1]), 0) + (2 * j + side) * slots
            pick = (ids == slot).astype(F32).astype(BF16)
            first = h * half + j * slots
            rows_ref[first:first + slots, :] = mm(pick, ratio).astype(BF16)


def finish_kernel(core_ref, energy_ref, weight_ref, inv_own_ref, inv_other_ref, lap_own_ref, lap_other_ref,
                  rows_ref, val_ref, lap_ref, out_ref, *, size):
    core = core_ref[0]
    half = lap_own_ref.shape[0]
    lap_part = mm_tn(lap_own_ref[...], rows_ref[:half, :]) + mm_tn(lap_other_ref[...], rows_ref[half:, :])
    mixed = energy_ref[0] * val_ref[...].astype(F32) - 0.5 * (lap_ref[...].astype(F32) - lap_part)
    mixed = (weight_ref[0] * mixed).astype(BF16)
    in_order(out_ref, mm(inv_own_ref[...], mixed), core, size)
    in_order(out_ref, mm(inv_other_ref[...], mixed), 1 - core, size)


VMEM = pl.BlockSpec(memory_space=pltpu.VMEM)
SMEM = pl.BlockSpec(memory_space=pltpu.SMEM)


def body(coefficients, inverse, cell_index, fraction, energies, weights, occupied):
    cells, width = coefficients.shape
    _, rows, electrons = inverse.shape
    shards = electrons // rows
    slots = 3 * electrons // (2 * shards)
    chips = ("xh", "z")
    me = (lax.axis_index(chips) * 2 + lax.axis_index("core")).astype(jnp.int32).reshape(1)
    core = lax.axis_index("core").astype(jnp.int32).reshape(1)
    swap = [(0, 1), (1, 0)]

    spread = jnp.broadcast_to(inverse, (shards // 2, rows, electrons))
    inv_own = lax.all_to_all(spread, chips, 0, 0, tiled=True).reshape(electrons // 2, electrons)

    out = lambda *shape_dtype: jax.ShapeDtypeStruct(*shape_dtype)
    val, lap, lap_slots, slot = pl.pallas_call(
        functools.partial(eval_kernel, shards=shards),
        out_shape=[
            out((electrons, width), BF16),
            out((electrons, width), BF16),
            out((slots, electrons), BF16),
            out((1, electrons), jnp.int32),
        ],
        in_specs=[SMEM, VMEM, VMEM, VMEM, VMEM],
        out_specs=[VMEM] * 4,
        scratch_shapes=[
            pltpu.VMEM((electrons, 8 * GRID), BF16),
            pltpu.VMEM((electrons, 8 * GRID), F32),
            pltpu.VMEM((8 * GRID, 4 * PLANE), BF16),
            pltpu.VMEM((2 * TILE, cells), BF16),
            pltpu.VMEM((2 * TILE, cells), BF16),
        ],
        compiler_params=pltpu.CompilerParams(vmem_limit_bytes=32 * 1024 * 1024),
        cost_estimate=pl.CostEstimate(
            flops=4 * electrons * cells * width, bytes_accessed=4 * cells * width, transcendentals=0
        ),
        name="evaluate",
    )(me, coefficients, cell_index[0], fraction[0], occupied.reshape(1, electrons))

    spread_lap = jnp.broadcast_to(lap_slots[None], (shards // 2, slots, electrons))
    lap_own = lax.all_to_all(spread_lap, chips, 0, 0, tiled=True).reshape(shards // 2 * slots, electrons)
    inv_other = lax.ppermute(inv_own, "core", swap)
    lap_other = lax.ppermute(lap_own, "core", swap)

    ratio_rows, _ = pl.pallas_call(
        functools.partial(ratio_kernel, slots=slots, size=rows),
        out_shape=[out((shards * slots, width), BF16), out((electrons, width), BF16)],
        in_specs=[SMEM] + [VMEM] * 4,
        out_specs=[VMEM] * 2,
        compiler_params=pltpu.CompilerParams(vmem_limit_bytes=24 * 1024 * 1024),
        cost_estimate=pl.CostEstimate(
            flops=5 * electrons * electrons * width, bytes_accessed=4 * electrons * electrons, transcendentals=0
        ),
        name="ratio",
    )(core, inv_own, inv_other, val, slot)

    partial = pl.pallas_call(
        functools.partial(finish_kernel, size=rows),
        out_shape=out((electrons, width), BF16),
        in_specs=[SMEM] * 3 + [VMEM] * 7,
        out_specs=VMEM,
        compiler_params=pltpu.CompilerParams(vmem_limit_bytes=32 * 1024 * 1024),
        cost_estimate=pl.CostEstimate(
            flops=5 * electrons * electrons * width, bytes_accessed=8 * electrons * electrons, transcendentals=0
        ),
        name="finish",
    )(core, energies, weights, inv_own, inv_other, lap_own, lap_other, ratio_rows, val, lap)

    walkers = ("y", "xl")
    count = lax.axis_size(walkers)
    blocks = lax.all_to_all(partial.reshape(count, electrons // count, width), walkers, 0, 0, tiled=True)
    return jnp.sum(blocks.astype(F32), axis=0)


def solution(mesh):
    fine = Mesh(mesh.devices.reshape(4, 2, 2, 4, 2), ("y", "xl", "xh", "z", "core"))
    walk, orb = ("y", "xl"), ("xh", "z", "core")
    in_specs = (
        P(None, orb),
        P(walk, orb, None),
        P(walk, None, None),
        P(walk, None, None),
        P(walk),
        P(walk),
        P(),
    )
    return jax.shard_map(body, mesh=fine, in_specs=in_specs, out_specs=P(walk, orb), check_vma=False)
```

```python
import functools

import jax
import jax.numpy as jnp
from jax import lax
from jax.experimental import pallas as pl
from jax.experimental.pallas import tpu as pltpu
from jax.sharding import Mesh
from jax.sharding import PartitionSpec as P


GRID = 16
PLANE = GRID * GRID
TILE = 256
BF16 = jnp.bfloat16
F32 = jnp.float32


def mm(left, right):
    return jnp.dot(left, right, preferred_element_type=F32)


def mm_nt(left, right):
    return lax.dot_general(left, right, (((1,), (1,)), ((), ())), preferred_element_type=F32)


def mm_tn(left, right):
    return lax.dot_general(left, right, (((0,), (0,)), ((), ())), preferred_element_type=F32)


def dense_rows(cell, frac):
    remain = 1.0 - frac
    square = frac * frac
    cubed = square * frac
    sixth = 1.0 / 6.0
    values = [
        remain * remain * remain * sixth,
        (3.0 * cubed - 6.0 * square + 4.0) * sixth,
        (-3.0 * cubed + 3.0 * square + 3.0 * frac + 1.0) * sixth,
        cubed * sixth,
    ]
    curves = [remain, 3.0 * frac - 2.0, 1.0 - 3.0 * frac, frac]
    line = lax.broadcasted_iota(jnp.int32, (GRID, cell.shape[1]), 0)
    tap = (line - cell + (GRID + 1)) & (GRID - 1)
    value = jnp.zeros((GRID, cell.shape[1]), F32)
    curve = jnp.zeros((GRID, cell.shape[1]), F32)
    for a in range(4):
        value = jnp.where(tap == a, values[a], value)
        curve = jnp.where(tap == a, curves[a], curve)
    return value, curve


def slot_tables(me, occ, shards, width, slots):
    owner = lax.broadcasted_iota(jnp.int32, (shards, occ.shape[1]), 0) == lax.div(occ, width)
    count = owner.astype(jnp.int32)
    lane = lax.broadcasted_iota(jnp.int32, count.shape, 1)
    step = 1
    while step < occ.shape[1]:
        count = count + jnp.where(lane >= step, pltpu.roll(count, step, 1), 0)
        step *= 2
    rank = jnp.sum(jnp.where(owner, count - 1, 0), axis=0, keepdims=True)
    slot = lax.div(occ, width) * slots + rank
    placed = lax.broadcasted_iota(jnp.int32, (slots, occ.shape[1]), 0) == slot - me * slots
    column = lax.broadcasted_iota(jnp.int32, (width, occ.shape[1]), 0) == occ - me * width
    picker = mm_nt(placed.astype(F32).astype(BF16), column.astype(F32).astype(BF16)).astype(BF16)
    return slot, picker


def expand(rows, weights):
    return jnp.concatenate([rows[g:g + 1, :] * weights for g in range(GRID)], axis=0)


def eval_kernel(*refs, shards, slots, first, electrons):
    if first == 0:
        me_ref, coef_ref, cell_ref, frac_ref, occ_ref, val_ref, lap_ref, lapt_ref, turned_ref, picker_ref, slot_ref, *weight_refs = refs
    else:
        turned_ref, picker_ref, cell_ref, frac_ref, val_ref, lap_ref, lapt_ref, *weight_refs = refs

    def build(t, value_ref, lap_ref):
        here = slice(first + t * TILE, first + (t + 1) * TILE)
        vx, cx = dense_rows(cell_ref[0, :, here], frac_ref[0, :, here])
        vy, cy = dense_rows(cell_ref[1, :, here], frac_ref[1, :, here])
        vz, cz = dense_rows(cell_ref[2, :, here], frac_ref[2, :, here])
        value = expand(vy, vz)
        curve = expand(cy, vz) + expand(vy, cz)
        for g in range(GRID):
            x_value, x_curve = vx[g:g + 1, :], cx[g:g + 1, :]
            value_ref[g * PLANE:(g + 1) * PLANE, :] = (x_value * value).astype(BF16)
            lap_ref[g * PLANE:(g + 1) * PLANE, :] = (x_curve * value + x_value * curve).astype(BF16)

    def product(t, value_w, lap_w):
        here = slice(t * TILE, (t + 1) * TILE)
        val_ref[:, here] = mm(turned_ref[...], value_w[...]).astype(BF16)
        lap = mm(turned_ref[...], lap_w[...]).astype(BF16)
        lap_ref[:, here] = lap
        lapt_ref[:, here] = mm(picker_ref[...], lap).astype(BF16)

    tiles = electrons // TILE
    build(0, weight_refs[0], weight_refs[1])
    if first == 0:
        slot, picker = slot_tables(me_ref[0], occ_ref[...], shards, coef_ref.shape[1], slots)
        slot_ref[...] = slot
        picker_ref[...] = picker
        for g in range(GRID):
            turned_ref[:, g * PLANE:(g + 1) * PLANE] = jnp.transpose(coef_ref[g * PLANE:(g + 1) * PLANE, :])
    for t in range(tiles):
        if t + 1 < tiles:
            build(t + 1, *weight_refs[2 * ((t + 1) % 2):][:2])
        product(t, *weight_refs[2 * (t % 2):][:2])


def owners(me_ref, z_count):
    me = me_ref[0]
    core = lax.rem(me, 2)
    z = lax.rem(lax.div(me, 2), z_count)
    plane = lax.div(me, 2 * z_count)
    chips = [(p * z_count + lax.rem(z + dz, z_count)) * 2
             for dz in (0, z_count - 1, 1, 2) for p in (plane, 1 - plane)]
    return [chip + core for chip in chips] + [chip + 1 - core for chip in chips]


def in_order(out_ref, value, blocks, size):
    for j, block in enumerate(blocks):
        start = pl.multiple_of(block * size, size)
        out_ref[pl.ds(start, size), :] = value[j * size:(j + 1) * size].astype(out_ref.dtype)


def inverse_times(inv_refs, right, out_ref, order, size):
    first = 0
    for ref in inv_refs:
        count = ref.shape[0] // size
        in_order(out_ref, mm_nt(ref[...], right), order[first:first + count], size)
        first += count


def ratio_kernel(me_ref, *refs, parts, z_count, slots, size):
    inv_refs, val_refs = refs[:parts], refs[parts:-3]
    slot_ref, rows_ref, ratio_ref = refs[-3:]
    order = owners(me_ref, z_count)
    val = jnp.concatenate([ref[...] for ref in val_refs], axis=1)
    inverse_times(inv_refs, val, ratio_ref, order, size)
    ratio = ratio_ref[...]
    slot = slot_ref[...]
    for j in range(0, len(order), 2):
        ids = lax.broadcasted_iota(jnp.int32, (slots, slot.shape[1]), 0)
        pick = jnp.concatenate([(ids + block * slots == slot).astype(F32) for block in order[j:j + 2]], axis=0)
        rows_ref[j * slots:(j + 2) * slots, :] = mm(pick.astype(BF16), ratio).astype(BF16)


def finish_kernel(me_ref, energy_ref, weight_ref, *refs, parts, halves, z_count, size):
    inv_refs, lapt_refs = refs[:parts], refs[parts:2 * parts]
    rows_ref = refs[2 * parts]
    val_refs, lap_refs = refs[2 * parts + 1:2 * parts + 1 + halves], refs[2 * parts + 1 + halves:2 * parts + 1 + 2 * halves]
    out_ref = refs[-1]
    total = None
    first = 0
    for ref in lapt_refs:
        term = mm_tn(rows_ref[first:first + ref.shape[0], :], ref[...])
        total = term if total is None else total + term
        first += ref.shape[0]
    val = jnp.concatenate([ref[...] for ref in val_refs], axis=1).astype(F32)
    lap = jnp.concatenate([ref[...] for ref in lap_refs], axis=1).astype(F32)
    mixed = (weight_ref[0] * (energy_ref[0] * val - 0.5 * (lap - total))).astype(BF16)
    inverse_times(inv_refs, mixed, out_ref, owners(me_ref, z_count), size)


VMEM = pl.BlockSpec(memory_space=pltpu.VMEM)
SMEM = pl.BlockSpec(memory_space=pltpu.SMEM)


def ring_swap(piece):
    return lax.ppermute(piece, "xh", [(0, 1), (1, 0)])


def ring_pass(piece, shift):
    count = lax.axis_size("z")
    return lax.ppermute(piece, "z", [(i, (i + shift) % count) for i in range(count)])


def core_swap(piece):
    return lax.ppermute(piece, "core", [(0, 1), (1, 0)])


def ring_parts(pair):
    half = pair.shape[0] // 2
    below = ring_pass(pair, 1)
    above = ring_pass(pair, -1)
    far_first = ring_pass(below[:half], 1)
    far_second = ring_pass(above[half:], -1)
    return [pair, below, above, far_first, far_second]


def gradient(coefficients, inverse, cell_index, fraction, energies, weights, occupied):
    cells, width = coefficients.shape
    _, rows, electrons = inverse.shape
    z_count = lax.axis_size("z")
    shards = 2 * z_count * 2
    slots = 3 * electrons // (2 * shards)
    xh, z, core = lax.axis_index("xh"), lax.axis_index("z"), lax.axis_index("core")
    me = ((xh * z_count + z) * 2 + core).astype(jnp.int32).reshape(1)

    out = lambda *shape_dtype: jax.ShapeDtypeStruct(*shape_dtype)
    halves = 2
    part = electrons // halves

    def evaluate(h, *operands):
        results = [out((width, part), BF16), out((width, part), BF16), out((slots, part), BF16)]
        if h == 0:
            results += [out((width, cells), BF16), out((slots, width), BF16), out((1, electrons), jnp.int32)]
        return pl.pallas_call(
            functools.partial(eval_kernel, shards=shards, slots=slots, first=h * part, electrons=part),
            out_shape=results,
            in_specs=[SMEM] + [VMEM] * 4 if h == 0 else [VMEM] * 4,
            out_specs=[VMEM] * len(results),
            scratch_shapes=[pltpu.VMEM((cells, TILE), BF16)] * 4,
            compiler_params=pltpu.CompilerParams(vmem_limit_bytes=32 * 1024 * 1024),
            cost_estimate=pl.CostEstimate(
                flops=4 * part * cells * width, bytes_accessed=4 * cells * width, transcendentals=0
            ),
            name="evaluate",
        )(*operands)

    cell_index, fraction = jnp.transpose(cell_index, (1, 0, 2)), jnp.transpose(fraction, (1, 0, 2))
    mine = inverse.reshape(rows, electrons)
    inv_far = ring_swap(mine)
    inv_pair = jnp.concatenate([mine, inv_far], axis=0)
    inv_ring = ring_parts(inv_pair)
    val_a, lap_a, lapt_a, turned, picker, slot = evaluate(
        0, me, coefficients, cell_index, fraction, occupied.reshape(1, electrons)
    )
    val_b, lap_b, lapt_b = evaluate(1, turned, picker, cell_index, fraction)
    vals, laps = [val_a, val_b], [lap_a, lap_b]
    lapt_mine = jnp.concatenate([lapt_a, lapt_b], axis=1)
    lapt_far = ring_swap(lapt_mine)
    lap_pair = jnp.concatenate([lapt_mine, lapt_far], axis=0)
    lap_ring = ring_parts(lap_pair)
    inv_all = inv_ring + [core_swap(piece) for piece in inv_ring]
    lap_all = lap_ring + [core_swap(piece) for piece in lap_ring]
    parts = len(inv_all)

    ratio_rows, _ = pl.pallas_call(
        functools.partial(ratio_kernel, parts=parts, z_count=z_count, slots=slots, size=rows),
        out_shape=[out((shards * slots, width), BF16), out((electrons, width), BF16)],
        in_specs=[SMEM] + [VMEM] * (parts + 3),
        out_specs=[VMEM] * 2,
        compiler_params=pltpu.CompilerParams(vmem_limit_bytes=24 * 1024 * 1024),
        cost_estimate=pl.CostEstimate(
            flops=5 * electrons * electrons * width, bytes_accessed=4 * electrons * electrons, transcendentals=0
        ),
        name="ratio",
    )(me, *inv_all, *vals, slot)

    partial = pl.pallas_call(
        functools.partial(finish_kernel, parts=parts, halves=halves, z_count=z_count, size=rows),
        out_shape=out((electrons, width), BF16),
        in_specs=[SMEM] * 3 + [VMEM] * (2 * parts + 1 + 2 * halves),
        out_specs=VMEM,
        compiler_params=pltpu.CompilerParams(vmem_limit_bytes=32 * 1024 * 1024),
        cost_estimate=pl.CostEstimate(
            flops=5 * electrons * electrons * width, bytes_accessed=8 * electrons * electrons, transcendentals=0
        ),
        name="finish",
    )(me, energies, weights, *inv_all, *lap_all, ratio_rows, *vals, *laps)

    walkers = ("y", "xl")
    count = lax.axis_size(walkers)
    blocks = lax.all_to_all(partial.reshape(count, electrons // count, width), walkers, 0, 0, tiled=True)
    return jnp.sum(blocks.astype(F32), axis=0)


def solution(mesh):
    fine = Mesh(mesh.devices.reshape(4, 2, 2, 4, 2), ("y", "xl", "xh", "z", "core"))
    walk, orb = ("y", "xl"), ("xh", "z", "core")
    in_specs = (
        P(None, orb),
        P(walk, orb, None),
        P(walk, None, None),
        P(walk, None, None),
        P(walk),
        P(walk),
        P(),
    )
    return jax.shard_map(gradient, mesh=fine, in_specs=in_specs, out_specs=P(walk, orb), check_vma=False)
```

```python
import functools

import jax
import jax.numpy as jnp
from jax import lax
from jax.experimental import pallas as pl
from jax.experimental.pallas import tpu as pltpu
from jax.sharding import Mesh
from jax.sharding import PartitionSpec as P


GRID = 16
PLANE = GRID * GRID
TILE = 256
BF16 = jnp.bfloat16
F32 = jnp.float32


def mm(left, right):
    return jnp.dot(left, right, preferred_element_type=F32)


def mm_nt(left, right):
    return lax.dot_general(left, right, (((1,), (1,)), ((), ())), preferred_element_type=F32)


def mm_tn(left, right):
    return lax.dot_general(left, right, (((0,), (0,)), ((), ())), preferred_element_type=F32)


def dense_rows(cell, frac):
    remain = 1.0 - frac
    square = frac * frac
    cubed = square * frac
    sixth = 1.0 / 6.0
    values = [
        remain * remain * remain * sixth,
        (3.0 * cubed - 6.0 * square + 4.0) * sixth,
        (-3.0 * cubed + 3.0 * square + 3.0 * frac + 1.0) * sixth,
        cubed * sixth,
    ]
    curves = [remain, 3.0 * frac - 2.0, 1.0 - 3.0 * frac, frac]
    line = lax.broadcasted_iota(jnp.int32, (GRID, cell.shape[1]), 0)
    tap = (line - cell + (GRID + 1)) & (GRID - 1)
    value = jnp.zeros((GRID, cell.shape[1]), F32)
    curve = jnp.zeros((GRID, cell.shape[1]), F32)
    for a in range(4):
        value = jnp.where(tap == a, values[a], value)
        curve = jnp.where(tap == a, curves[a], curve)
    return value, curve


def slot_tables(me, occ, shards, width, slots):
    owner = lax.broadcasted_iota(jnp.int32, (shards, occ.shape[1]), 0) == lax.div(occ, width)
    count = owner.astype(jnp.int32)
    lane = lax.broadcasted_iota(jnp.int32, count.shape, 1)
    step = 1
    while step < occ.shape[1]:
        count = count + jnp.where(lane >= step, pltpu.roll(count, step, 1), 0)
        step *= 2
    rank = jnp.sum(jnp.where(owner, count - 1, 0), axis=0, keepdims=True)
    slot = lax.div(occ, width) * slots + rank
    placed = lax.broadcasted_iota(jnp.int32, (slots, occ.shape[1]), 0) == slot - me * slots
    column = lax.broadcasted_iota(jnp.int32, (width, occ.shape[1]), 0) == occ - me * width
    picker = mm_nt(placed.astype(F32).astype(BF16), column.astype(F32).astype(BF16)).astype(BF16)
    return slot, picker


def expand(rows, weights):
    return jnp.concatenate([rows[g:g + 1, :] * weights for g in range(GRID)], axis=0)


def turn_kernel(coef_hbm, turned_ref, coef_ref, sems):
    pieces = sems.shape[0]
    rows = coef_ref.shape[0] // pieces
    copies = [
        pltpu.make_async_copy(coef_hbm.at[pl.ds(k * rows, rows)], coef_ref.at[pl.ds(k * rows, rows)], sems.at[k])
        for k in range(pieces)
    ]
    for copy in copies:
        copy.start()
    for k, copy in enumerate(copies):
        copy.wait()
        for first in range(k * rows, (k + 1) * rows, PLANE):
            turned_ref[:, first:first + PLANE] = jnp.transpose(coef_ref[first:first + PLANE, :])


def eval_kernel(*refs, shards, slots, first, electrons):
    if first == 0:
        me_ref, turned_ref, cell_ref, frac_ref, occ_ref, val_ref, lap_ref, lapt_ref, picker_ref, slot_ref, *weight_refs = refs
    else:
        turned_ref, cell_ref, frac_ref, picker_ref, val_ref, lap_ref, lapt_ref, *weight_refs = refs

    def build(t, value_ref, lap_ref):
        here = slice(first + t * TILE, first + (t + 1) * TILE)
        vx, cx = dense_rows(cell_ref[0, :, here], frac_ref[0, :, here])
        vy, cy = dense_rows(cell_ref[1, :, here], frac_ref[1, :, here])
        vz, cz = dense_rows(cell_ref[2, :, here], frac_ref[2, :, here])
        value = expand(vy, vz)
        curve = expand(cy, vz) + expand(vy, cz)
        for g in range(GRID):
            x_value, x_curve = vx[g:g + 1, :], cx[g:g + 1, :]
            value_ref[g * PLANE:(g + 1) * PLANE, :] = (x_value * value).astype(BF16)
            lap_ref[g * PLANE:(g + 1) * PLANE, :] = (x_curve * value + x_value * curve).astype(BF16)

    def product(t, value_w, lap_w):
        here = slice(t * TILE, (t + 1) * TILE)
        val_ref[:, here] = mm(turned_ref[...], value_w[...]).astype(BF16)
        lap = mm(turned_ref[...], lap_w[...]).astype(BF16)
        lap_ref[:, here] = lap
        lapt_ref[:, here] = mm(picker_ref[...], lap).astype(BF16)

    tiles = electrons // TILE
    build(0, weight_refs[0], weight_refs[1])
    if first == 0:
        slot, picker = slot_tables(me_ref[0], occ_ref[...], shards, turned_ref.shape[0], slots)
        slot_ref[...] = slot
        picker_ref[...] = picker
    for t in range(tiles):
        if t + 1 < tiles:
            build(t + 1, *weight_refs[2 * ((t + 1) % 2):][:2])
        product(t, *weight_refs[2 * (t % 2):][:2])


def place(me_ref, z_count):
    me = me_ref[0]
    core = lax.rem(me, 2)
    z = lax.rem(lax.div(me, 2), z_count)
    plane = lax.div(me, 2 * z_count)
    along = [lax.rem(z + dz, z_count) for dz in (0, z_count - 1, 1, 2)]
    return plane, along, core


def inverse_times(me_ref, z_count, inv_refs, right, out_ref, size):
    plane, along, core = place(me_ref, z_count)
    blocks = [(p * z_count + z) * 2 + c for c in (core, 1 - core) for p in (plane, 1 - plane) for z in along]
    first = 0
    for ref in inv_refs:
        value = mm_nt(ref[...], right).astype(out_ref.dtype)
        count = ref.shape[0] // size
        for j, block in enumerate(blocks[first:first + count]):
            start = pl.multiple_of(block * size, size)
            out_ref[pl.ds(start, size), :] = value[j * size:(j + 1) * size]
        first += count


def ratio_kernel(me_ref, *refs, parts, z_count, slots, size):
    inv_refs, val_refs = refs[:parts], refs[parts:-3]
    slot_ref, rows_ref, ratio_ref = refs[-3:]
    val = jnp.concatenate([ref[...] for ref in val_refs], axis=1)
    inverse_times(me_ref, z_count, inv_refs, val, ratio_ref, size)
    ratio = ratio_ref[...]
    slot = slot_ref[...]
    plane, along, core = place(me_ref, z_count)
    blocks = [(p * z_count + z) * 2 + c for c in (core, 1 - core) for z in along for p in (plane, 1 - plane)]
    for j in range(0, len(blocks), 2):
        ids = lax.broadcasted_iota(jnp.int32, (slots, slot.shape[1]), 0)
        pick = jnp.concatenate([(ids + block * slots == slot).astype(F32) for block in blocks[j:j + 2]], axis=0)
        rows_ref[j * slots:(j + 2) * slots, :] = mm(pick.astype(BF16), ratio).astype(BF16)


def coupled(rows_ref, pieces):
    total = None
    for first, ref in pieces:
        term = mm_tn(rows_ref[first:first + ref.shape[0], :], ref[...])
        total = term if total is None else total + term
    return total


def couple_kernel(energy_ref, weight_ref, *refs, firsts):
    near_refs = refs[:len(firsts)]
    rows_ref, val_a, val_b, lap_a, lap_b, mixed_ref = refs[len(firsts):]
    total = coupled(rows_ref, list(zip(firsts, near_refs)))
    val = jnp.concatenate([val_a[...], val_b[...]], axis=1).astype(F32)
    lap = jnp.concatenate([lap_a[...], lap_b[...]], axis=1).astype(F32)
    mixed_ref[...] = weight_ref[0] * (energy_ref[0] * val - 0.5 * (lap - total))


def finish_kernel(me_ref, weight_ref, mixed_ref, rows_ref, *refs, firsts, z_count, size):
    far_refs, inv_refs, out_ref = refs[:len(firsts)], refs[len(firsts):-1], refs[-1]
    total = coupled(rows_ref, list(zip(firsts, far_refs)))
    mixed = (mixed_ref[...] + (0.5 * weight_ref[0]) * total).astype(BF16)
    inverse_times(me_ref, z_count, inv_refs, mixed, out_ref, size)


VMEM = pl.BlockSpec(memory_space=pltpu.VMEM)
SMEM = pl.BlockSpec(memory_space=pltpu.SMEM)
HBM = pl.BlockSpec(memory_space=pltpu.HBM)


def ring_swap(piece):
    return lax.ppermute(piece, "xh", [(0, 1), (1, 0)])


def ring_pass(piece, shift):
    count = lax.axis_size("z")
    return lax.ppermute(piece, "z", [(i, (i + shift) % count) for i in range(count)])


def core_swap(piece):
    return lax.ppermute(piece, "core", [(0, 1), (1, 0)])


def gradient(coefficients, inverse, cell_index, fraction, energies, weights, occupied):
    cells, width = coefficients.shape
    _, rows, electrons = inverse.shape
    z_count = lax.axis_size("z")
    shards = 2 * z_count * 2
    slots = 3 * electrons // (2 * shards)
    xh, z, core = lax.axis_index("xh"), lax.axis_index("z"), lax.axis_index("core")
    me = ((xh * z_count + z) * 2 + core).astype(jnp.int32).reshape(1)

    out = lambda *shape_dtype: jax.ShapeDtypeStruct(*shape_dtype)
    halves = 2
    part = electrons // halves

    def params(mib):
        return pltpu.CompilerParams(vmem_limit_bytes=mib * 1024 * 1024)

    def cost(products):
        return pl.CostEstimate(flops=2 * products, bytes_accessed=2 * cells * width, transcendentals=0)

    def evaluate(h, *operands):
        results = [out((width, part), BF16), out((width, part), BF16), out((slots, part), BF16)]
        if h == 0:
            results += [out((slots, width), BF16), out((1, electrons), jnp.int32)]
        return pl.pallas_call(
            functools.partial(eval_kernel, shards=shards, slots=slots, first=h * part, electrons=part),
            out_shape=results,
            in_specs=[SMEM] + [VMEM] * 4 if h == 0 else [VMEM] * 4,
            out_specs=[VMEM] * len(results),
            scratch_shapes=[pltpu.VMEM((cells, TILE), BF16)] * 4,
            compiler_params=params(32),
            cost_estimate=cost(2 * part * cells * width),
            name="evaluate",
        )(*operands)

    cell_index, fraction = jnp.transpose(cell_index, (1, 0, 2)), jnp.transpose(fraction, (1, 0, 2))
    mine = inverse.reshape(rows, electrons)
    half = rows // 2

    inv_below = ring_pass(mine, 1)
    inv_above = ring_pass(mine, -1)
    inv_far_mine = ring_swap(mine)
    inv_first = ring_pass(inv_below[:half], 1)
    inv_second = ring_pass(inv_above[half:], -1)
    inv_plane = jnp.concatenate([mine, inv_below, inv_above, inv_first, inv_second], axis=0)
    inv_far_rest = ring_swap(inv_plane[rows:])
    inv_own = [inv_plane, inv_far_mine, inv_far_rest]
    inv_others = [core_swap(inv_plane), core_swap(inv_far_mine)]
    inv_others.append(core_swap(inv_far_rest))
    inv_all = inv_own + inv_others

    turned = pl.pallas_call(
        turn_kernel,
        out_shape=out((width, cells), BF16),
        in_specs=[HBM],
        out_specs=VMEM,
        scratch_shapes=[pltpu.VMEM((cells, width), BF16), pltpu.SemaphoreType.DMA((4,))],
        compiler_params=params(50),
        cost_estimate=cost(cells * width * 64),
        name="turn",
    )(coefficients)
    val_a, lap_a, lapt_a, picker, slot = evaluate(0, me, turned, cell_index, fraction, occupied.reshape(1, electrons))
    val_b, lap_b, lapt_b = evaluate(1, turned, cell_index, fraction, picker)

    lapt_mine = jnp.concatenate([lapt_a, lapt_b], axis=1)
    lapt_far = ring_swap(lapt_mine)
    lap_pair = jnp.concatenate([lapt_mine, lapt_far], axis=0)
    lap_below = ring_pass(lap_pair, 1)
    lap_above = ring_pass(lap_pair, -1)
    lap_first = ring_pass(lap_below[:slots], 1)
    lap_second = ring_pass(lap_above[slots:], -1)
    near = [lap_pair, lap_below, lap_above]
    far = [lap_first, lap_second]
    near += [core_swap(piece) for piece in near]
    far += [core_swap(piece) for piece in far]
    total = shards * slots
    near_firsts = [0, 2 * slots, 4 * slots]
    near_firsts += [first + total // 2 for first in near_firsts]
    far_firsts = [6 * slots, 7 * slots]
    far_firsts += [first + total // 2 for first in far_firsts]

    ratio_rows, _ = pl.pallas_call(
        functools.partial(ratio_kernel, parts=len(inv_all), z_count=z_count, slots=slots, size=rows),
        out_shape=[out((total, width), BF16), out((electrons, width), BF16)],
        in_specs=[SMEM] + [VMEM] * (len(inv_all) + 3),
        out_specs=[VMEM] * 2,
        compiler_params=params(24),
        cost_estimate=cost(3 * electrons * electrons * width),
        name="ratio",
    )(me, *inv_all, val_a, val_b, slot)

    mixed = pl.pallas_call(
        functools.partial(couple_kernel, firsts=near_firsts),
        out_shape=out((width, electrons), F32),
        in_specs=[SMEM] * 2 + [VMEM] * (len(near) + 5),
        out_specs=VMEM,
        compiler_params=params(24),
        cost_estimate=cost(electrons * electrons * width),
        name="couple",
    )(energies, weights, *near, ratio_rows, val_a, val_b, lap_a, lap_b)

    partial = pl.pallas_call(
        functools.partial(finish_kernel, firsts=far_firsts, z_count=z_count, size=rows),
        out_shape=out((electrons, width), BF16),
        in_specs=[SMEM] * 2 + [VMEM] * (2 + len(far) + len(inv_all)),
        out_specs=VMEM,
        compiler_params=params(24),
        cost_estimate=cost(electrons * electrons * width),
        name="finish",
    )(me, weights, mixed, ratio_rows, *far, *inv_all)

    walkers = ("y", "xl")
    count = lax.axis_size(walkers)
    blocks = lax.all_to_all(partial.reshape(count, electrons // count, width), walkers, 0, 0, tiled=True)
    return jnp.sum(blocks.astype(F32), axis=0)


def solution(mesh):
    fine = Mesh(mesh.devices.reshape(4, 2, 2, 4, 2), ("y", "xl", "xh", "z", "core"))
    walk, orb = ("y", "xl"), ("xh", "z", "core")
    in_specs = (
        P(None, orb),
        P(walk, orb, None),
        P(walk, None, None),
        P(walk, None, None),
        P(walk),
        P(walk),
        P(),
    )
    return jax.shard_map(gradient, mesh=fine, in_specs=in_specs, out_specs=P(walk, orb), check_vma=False)
```

```python
import functools

import jax
import jax.numpy as jnp
from jax import lax
from jax.experimental import pallas as pl
from jax.experimental.pallas import tpu as pltpu
from jax.sharding import Mesh
from jax.sharding import PartitionSpec as P


GRID = 16
PLANE = GRID * GRID
TILE = 256
BF16 = jnp.bfloat16
F32 = jnp.float32


def mm(left, right):
    return jnp.dot(left, right, preferred_element_type=F32)


def mm_nt(left, right):
    return lax.dot_general(left, right, (((1,), (1,)), ((), ())), preferred_element_type=F32)


def mm_tn(left, right):
    return lax.dot_general(left, right, (((0,), (0,)), ((), ())), preferred_element_type=F32)


def dense_rows(cell, frac):
    remain = 1.0 - frac
    square = frac * frac
    cubed = square * frac
    sixth = 1.0 / 6.0
    values = [
        remain * remain * remain * sixth,
        (3.0 * cubed - 6.0 * square + 4.0) * sixth,
        (-3.0 * cubed + 3.0 * square + 3.0 * frac + 1.0) * sixth,
        cubed * sixth,
    ]
    curves = [remain, 3.0 * frac - 2.0, 1.0 - 3.0 * frac, frac]
    line = lax.broadcasted_iota(jnp.int32, (GRID, cell.shape[1]), 0)
    tap = (line - cell + (GRID + 1)) & (GRID - 1)
    value = jnp.zeros((GRID, cell.shape[1]), F32)
    curve = jnp.zeros((GRID, cell.shape[1]), F32)
    for a in range(4):
        value = jnp.where(tap == a, values[a], value)
        curve = jnp.where(tap == a, curves[a], curve)
    return value, curve


def slot_tables(me, occ, shards, width, slots):
    owner = lax.broadcasted_iota(jnp.int32, (shards, occ.shape[1]), 0) == lax.div(occ, width)
    count = owner.astype(jnp.int32)
    lane = lax.broadcasted_iota(jnp.int32, count.shape, 1)
    step = 1
    while step < occ.shape[1]:
        count = count + jnp.where(lane >= step, pltpu.roll(count, step, 1), 0)
        step *= 2
    rank = jnp.sum(jnp.where(owner, count - 1, 0), axis=0, keepdims=True)
    slot = lax.div(occ, width) * slots + rank
    placed = lax.broadcasted_iota(jnp.int32, (slots, occ.shape[1]), 0) == slot - me * slots
    column = lax.broadcasted_iota(jnp.int32, (width, occ.shape[1]), 0) == occ - me * width
    picker = mm_nt(placed.astype(F32).astype(BF16), column.astype(F32).astype(BF16)).astype(BF16)
    return slot, picker


def expand(rows, weights):
    return jnp.concatenate([rows[g:g + 1, :] * weights for g in range(GRID)], axis=0)


def turn_kernel(coef_hbm, turned_ref, coef_ref, sems):
    pieces = sems.shape[0]
    rows = coef_ref.shape[0] // pieces
    copies = [
        pltpu.make_async_copy(coef_hbm.at[pl.ds(k * rows, rows)], coef_ref.at[pl.ds(k * rows, rows)], sems.at[k])
        for k in range(pieces)
    ]
    for copy in copies:
        copy.start()
    for k, copy in enumerate(copies):
        copy.wait()
        for first in range(k * rows, (k + 1) * rows, PLANE):
            turned_ref[:, first:first + PLANE] = jnp.transpose(coef_ref[first:first + PLANE, :])


def weight_tables(cell_ref, frac_ref, here):
    tables = [dense_rows(cell_ref[k, :, here], frac_ref[k, :, here]) for k in range(3)]
    (vx, cx), (vy, cy), (vz, cz) = tables
    return vx, cx, expand(vy, vz), expand(cy, vz) + expand(vy, cz)


def build_laplacian(tables, w_ref):
    vx, cx, value, curve = tables
    for g in range(GRID):
        w_ref[g * PLANE:(g + 1) * PLANE, :] = (cx[g:g + 1, :] * value + vx[g:g + 1, :] * curve).astype(BF16)


def build_value(tables, w_ref):
    vx, _, value, _ = tables
    for g in range(GRID):
        w_ref[g * PLANE:(g + 1) * PLANE, :] = (vx[g:g + 1, :] * value).astype(BF16)


def early_kernel(me_ref, turned_ref, cell_ref, frac_ref, occ_ref, lapt_ref, slot_ref, *w_refs, shards):
    slots, electrons = lapt_ref.shape
    slot, picker = slot_tables(me_ref[0], occ_ref[...], shards, turned_ref.shape[0], slots)
    slot_ref[...] = slot
    chosen = mm(picker, turned_ref[...]).astype(BF16)
    tiles = [slice(first, first + TILE) for first in range(0, electrons, TILE)]
    build_laplacian(weight_tables(cell_ref, frac_ref, tiles[0]), w_refs[0])
    for t, here in enumerate(tiles):
        if t + 1 < len(tiles):
            build_laplacian(weight_tables(cell_ref, frac_ref, tiles[t + 1]), w_refs[(t + 1) % 2])
        lapt_ref[:, here] = mm(chosen, w_refs[t % 2][...]).astype(BF16)


def eval_kernel(turned_ref, cell_ref, frac_ref, val_ref, lap_ref, *w_refs, first):
    electrons = val_ref.shape[1]

    def build(t):
        tables = weight_tables(cell_ref, frac_ref, slice(first + t * TILE, first + (t + 1) * TILE))
        build_value(tables, w_refs[2 * (t % 2)])
        build_laplacian(tables, w_refs[2 * (t % 2) + 1])

    build(0)
    for t in range(electrons // TILE):
        if (t + 1) * TILE < electrons:
            build(t + 1)
        here = slice(t * TILE, (t + 1) * TILE)
        val_ref[:, here] = mm(turned_ref[...], w_refs[2 * (t % 2)][...]).astype(BF16)
        lap_ref[:, here] = mm(turned_ref[...], w_refs[2 * (t % 2) + 1][...]).astype(BF16)


def place(me_ref, z_count):
    me = me_ref[0]
    core = lax.rem(me, 2)
    z = lax.rem(lax.div(me, 2), z_count)
    plane = lax.div(me, 2 * z_count)
    along = [lax.rem(z + dz, z_count) for dz in (0, z_count - 1, 1, 2)]
    return plane, along, core


def inverse_times(me_ref, z_count, inv_refs, right, out_ref, size):
    plane, along, core = place(me_ref, z_count)
    blocks = [(p * z_count + z) * 2 + c for c in (core, 1 - core) for p in (plane, 1 - plane) for z in along]
    first = 0
    for ref in inv_refs:
        value = mm_nt(ref[...], right).astype(out_ref.dtype)
        count = ref.shape[0] // size
        for j, block in enumerate(blocks[first:first + count]):
            start = pl.multiple_of(block * size, size)
            out_ref[pl.ds(start, size), :] = value[j * size:(j + 1) * size]
        first += count


def ratio_kernel(me_ref, *refs, parts, z_count, slots, size):
    inv_refs, val_refs = refs[:parts], refs[parts:-3]
    slot_ref, rows_ref, ratio_ref = refs[-3:]
    val = jnp.concatenate([ref[...] for ref in val_refs], axis=1)
    inverse_times(me_ref, z_count, inv_refs, val, ratio_ref, size)
    ratio = ratio_ref[...]
    slot = slot_ref[...]
    plane, along, core = place(me_ref, z_count)
    blocks = [(p * z_count + z) * 2 + c for c in (core, 1 - core) for z in along for p in (plane, 1 - plane)]
    for j in range(0, len(blocks), 2):
        ids = lax.broadcasted_iota(jnp.int32, (slots, slot.shape[1]), 0)
        pick = jnp.concatenate([(ids + block * slots == slot).astype(F32) for block in blocks[j:j + 2]], axis=0)
        rows_ref[j * slots:(j + 2) * slots, :] = mm(pick.astype(BF16), ratio).astype(BF16)


def coupled(rows_ref, pieces):
    total = None
    for first, ref in pieces:
        term = mm_tn(rows_ref[first:first + ref.shape[0], :], ref[...])
        total = term if total is None else total + term
    return total


def couple_kernel(energy_ref, weight_ref, *refs, firsts):
    near_refs = refs[:len(firsts)]
    rows_ref, val_a, val_b, lap_a, lap_b, mixed_ref = refs[len(firsts):]
    total = coupled(rows_ref, list(zip(firsts, near_refs)))
    val = jnp.concatenate([val_a[...], val_b[...]], axis=1).astype(F32)
    lap = jnp.concatenate([lap_a[...], lap_b[...]], axis=1).astype(F32)
    mixed_ref[...] = weight_ref[0] * (energy_ref[0] * val - 0.5 * (lap - total))


def finish_kernel(me_ref, weight_ref, mixed_ref, rows_ref, *refs, firsts, z_count, size):
    far_refs, inv_refs, out_ref = refs[:len(firsts)], refs[len(firsts):-1], refs[-1]
    total = coupled(rows_ref, list(zip(firsts, far_refs)))
    mixed = (mixed_ref[...] + (0.5 * weight_ref[0]) * total).astype(BF16)
    inverse_times(me_ref, z_count, inv_refs, mixed, out_ref, size)


VMEM = pl.BlockSpec(memory_space=pltpu.VMEM)
SMEM = pl.BlockSpec(memory_space=pltpu.SMEM)
HBM = pl.BlockSpec(memory_space=pltpu.HBM)


def ring_swap(piece):
    return lax.ppermute(piece, "xh", [(0, 1), (1, 0)])


def ring_pass(piece, shift):
    count = lax.axis_size("z")
    return lax.ppermute(piece, "z", [(i, (i + shift) % count) for i in range(count)])


def core_swap(piece):
    return lax.ppermute(piece, "core", [(0, 1), (1, 0)])


def gradient(coefficients, inverse, cell_index, fraction, energies, weights, occupied):
    cells, width = coefficients.shape
    _, rows, electrons = inverse.shape
    z_count = lax.axis_size("z")
    shards = 2 * z_count * 2
    slots = 3 * electrons // (2 * shards)
    xh, z, core = lax.axis_index("xh"), lax.axis_index("z"), lax.axis_index("core")
    me = ((xh * z_count + z) * 2 + core).astype(jnp.int32).reshape(1)

    out = lambda *shape_dtype: jax.ShapeDtypeStruct(*shape_dtype)
    halves = 2
    part = electrons // halves

    def params(mib):
        return pltpu.CompilerParams(vmem_limit_bytes=mib * 1024 * 1024)

    def cost(products):
        return pl.CostEstimate(flops=2 * products, bytes_accessed=2 * cells * width, transcendentals=0)

    def evaluate(h):
        return pl.pallas_call(
            functools.partial(eval_kernel, first=h * part),
            out_shape=[out((width, part), BF16)] * 2,
            in_specs=[VMEM] * 3,
            out_specs=[VMEM] * 2,
            scratch_shapes=[pltpu.VMEM((cells, TILE), BF16)] * 4,
            compiler_params=params(32),
            cost_estimate=cost(2 * part * cells * width),
            name="evaluate",
        )(turned, cell_index, fraction)

    cell_index, fraction = jnp.transpose(cell_index, (1, 0, 2)), jnp.transpose(fraction, (1, 0, 2))
    mine = inverse.reshape(rows, electrons)
    half = rows // 2

    inv_below = ring_pass(mine, 1)
    inv_above = ring_pass(mine, -1)
    inv_far_mine = ring_swap(mine)
    inv_first = ring_pass(inv_below[:half], 1)
    inv_second = ring_pass(inv_above[half:], -1)
    inv_rest = jnp.concatenate([inv_below, inv_above, inv_first, inv_second], axis=0)
    inv_far_rest = ring_swap(inv_rest)
    inv_others = [core_swap(mine), core_swap(inv_rest), core_swap(inv_far_mine)]
    inv_others.append(core_swap(inv_far_rest))
    inv_all = [mine, inv_rest, inv_far_mine, inv_far_rest] + inv_others

    turned = pl.pallas_call(
        turn_kernel,
        out_shape=out((width, cells), BF16),
        in_specs=[HBM],
        out_specs=VMEM,
        scratch_shapes=[pltpu.VMEM((cells, width), BF16), pltpu.SemaphoreType.DMA((4,))],
        compiler_params=params(50),
        cost_estimate=cost(cells * width * 64),
        name="turn",
    )(coefficients)
    lapt_mine, slot = pl.pallas_call(
        functools.partial(early_kernel, shards=shards),
        out_shape=[out((slots, electrons), BF16), out((1, electrons), jnp.int32)],
        in_specs=[SMEM] + [VMEM] * 4,
        out_specs=[VMEM] * 2,
        scratch_shapes=[pltpu.VMEM((cells, TILE), BF16)] * 2,
        compiler_params=params(32),
        cost_estimate=cost(slots * cells * electrons),
        name="early",
    )(me, turned, cell_index, fraction, occupied.reshape(1, electrons))
    val_a, lap_a = evaluate(0)
    val_b, lap_b = evaluate(1)

    lapt_far = ring_swap(lapt_mine)
    lap_pair = jnp.concatenate([lapt_mine, lapt_far], axis=0)
    lap_below = ring_pass(lap_pair, 1)
    lap_above = ring_pass(lap_pair, -1)
    lap_first = ring_pass(lap_below[:slots], 1)
    lap_second = ring_pass(lap_above[slots:], -1)
    near = [lap_pair, lap_below, lap_above]
    far = [lap_first, lap_second]
    near += [core_swap(piece) for piece in near]
    far += [core_swap(piece) for piece in far]
    total = shards * slots
    near_firsts = [0, 2 * slots, 4 * slots]
    near_firsts += [first + total // 2 for first in near_firsts]
    far_firsts = [6 * slots, 7 * slots]
    far_firsts += [first + total // 2 for first in far_firsts]

    ratio_rows, _ = pl.pallas_call(
        functools.partial(ratio_kernel, parts=len(inv_all), z_count=z_count, slots=slots, size=rows),
        out_shape=[out((total, width), BF16), out((electrons, width), BF16)],
        in_specs=[SMEM] + [VMEM] * (len(inv_all) + 3),
        out_specs=[VMEM] * 2,
        compiler_params=params(24),
        cost_estimate=cost(3 * electrons * electrons * width),
        name="ratio",
    )(me, *inv_all, val_a, val_b, slot)

    mixed = pl.pallas_call(
        functools.partial(couple_kernel, firsts=near_firsts),
        out_shape=out((width, electrons), F32),
        in_specs=[SMEM] * 2 + [VMEM] * (len(near) + 5),
        out_specs=VMEM,
        compiler_params=params(24),
        cost_estimate=cost(electrons * electrons * width),
        name="couple",
    )(energies, weights, *near, ratio_rows, val_a, val_b, lap_a, lap_b)

    partial = pl.pallas_call(
        functools.partial(finish_kernel, firsts=far_firsts, z_count=z_count, size=rows),
        out_shape=out((electrons, width), BF16),
        in_specs=[SMEM] * 2 + [VMEM] * (2 + len(far) + len(inv_all)),
        out_specs=VMEM,
        compiler_params=params(24),
        cost_estimate=cost(electrons * electrons * width),
        name="finish",
    )(me, weights, mixed, ratio_rows, *far, *inv_all)

    walkers = ("y", "xl")
    count = lax.axis_size(walkers)
    blocks = lax.all_to_all(partial.reshape(count, electrons // count, width), walkers, 0, 0, tiled=True)
    return jnp.sum(blocks.astype(F32), axis=0)


def solution(mesh):
    fine = Mesh(mesh.devices.reshape(4, 2, 2, 4, 2), ("y", "xl", "xh", "z", "core"))
    walk, orb = ("y", "xl"), ("xh", "z", "core")
    in_specs = (
        P(None, orb),
        P(walk, orb, None),
        P(walk, None, None),
        P(walk, None, None),
        P(walk),
        P(walk),
        P(),
    )
    return jax.shard_map(gradient, mesh=fine, in_specs=in_specs, out_specs=P(walk, orb), check_vma=False)
```

```python
import functools

import jax
import jax.numpy as jnp
from jax import lax
from jax.experimental import pallas as pl
from jax.experimental.pallas import tpu as pltpu
from jax.sharding import Mesh
from jax.sharding import PartitionSpec as P


GRID = 16
PLANE = GRID * GRID
TILE = 256
BF16 = jnp.bfloat16
F32 = jnp.float32


def mm(left, right):
    return jnp.dot(left, right, preferred_element_type=F32)


def mm_nt(left, right):
    return lax.dot_general(left, right, (((1,), (1,)), ((), ())), preferred_element_type=F32)


def mm_tn(left, right):
    return lax.dot_general(left, right, (((0,), (0,)), ((), ())), preferred_element_type=F32)


def dense_rows(cell, frac):
    remain = 1.0 - frac
    square = frac * frac
    cubed = square * frac
    sixth = 1.0 / 6.0
    values = [
        remain * remain * remain * sixth,
        (3.0 * cubed - 6.0 * square + 4.0) * sixth,
        (-3.0 * cubed + 3.0 * square + 3.0 * frac + 1.0) * sixth,
        cubed * sixth,
    ]
    curves = [remain, 3.0 * frac - 2.0, 1.0 - 3.0 * frac, frac]
    line = lax.broadcasted_iota(jnp.int32, (GRID, cell.shape[1]), 0)
    tap = (line - cell + (GRID + 1)) & (GRID - 1)
    value = jnp.zeros((GRID, cell.shape[1]), F32)
    curve = jnp.zeros((GRID, cell.shape[1]), F32)
    for a in range(4):
        value = jnp.where(tap == a, values[a], value)
        curve = jnp.where(tap == a, curves[a], curve)
    return value, curve


def slot_tables(me, occ, shards, width, slots):
    owner = lax.broadcasted_iota(jnp.int32, (shards, occ.shape[1]), 0) == lax.div(occ, width)
    count = owner.astype(jnp.int32)
    lane = lax.broadcasted_iota(jnp.int32, count.shape, 1)
    step = 1
    while step < occ.shape[1]:
        count = count + jnp.where(lane >= step, pltpu.roll(count, step, 1), 0)
        step *= 2
    rank = jnp.sum(jnp.where(owner, count - 1, 0), axis=0, keepdims=True)
    slot = lax.div(occ, width) * slots + rank
    placed = lax.broadcasted_iota(jnp.int32, (slots, occ.shape[1]), 0) == slot - me * slots
    column = lax.broadcasted_iota(jnp.int32, (width, occ.shape[1]), 0) == occ - me * width
    picker = mm_nt(placed.astype(F32).astype(BF16), column.astype(F32).astype(BF16)).astype(BF16)
    return slot, picker


def expand(rows, weights):
    return jnp.concatenate([rows[g:g + 1, :] * weights for g in range(GRID)], axis=0)


def turn_kernel(coef_hbm, turned_ref, coef_ref, sems):
    pieces = sems.shape[0]
    rows = coef_ref.shape[0] // pieces
    copies = [
        pltpu.make_async_copy(coef_hbm.at[pl.ds(k * rows, rows)], coef_ref.at[pl.ds(k * rows, rows)], sems.at[k])
        for k in range(pieces)
    ]
    for copy in copies:
        copy.start()
    for k, copy in enumerate(copies):
        copy.wait()
        for first in range(k * rows, (k + 1) * rows, PLANE):
            turned_ref[:, first:first + PLANE] = jnp.transpose(coef_ref[first:first + PLANE, :])


def weight_tables(cell_ref, frac_ref, here):
    tables = [dense_rows(cell_ref[k, :, here], frac_ref[k, :, here]) for k in range(3)]
    (vx, cx), (vy, cy), (vz, cz) = tables
    return vx, cx, expand(vy, vz), expand(cy, vz) + expand(vy, cz)


def build_laplacian(tables, w_ref):
    vx, cx, value, curve = tables
    for g in range(GRID):
        w_ref[g * PLANE:(g + 1) * PLANE, :] = (cx[g:g + 1, :] * value + vx[g:g + 1, :] * curve).astype(BF16)


def build_value(tables, w_ref):
    vx, _, value, _ = tables
    for g in range(GRID):
        w_ref[g * PLANE:(g + 1) * PLANE, :] = (vx[g:g + 1, :] * value).astype(BF16)


def early_kernel(turned_ref, cell_ref, frac_ref, occ_ref, lapt_ref, slot_ref, *w_refs, shards):
    slots, electrons = lapt_ref.shape
    plane, along, core = place(shards // 4)
    me = (plane * (shards // 4) + along[0]) * 2 + core
    slot, picker = slot_tables(me, occ_ref[...], shards, turned_ref.shape[0], slots)
    slot_ref[...] = slot
    chosen = mm(picker, turned_ref[...]).astype(BF16)
    tiles = [slice(first, first + TILE) for first in range(0, electrons, TILE)]
    build_laplacian(weight_tables(cell_ref, frac_ref, tiles[0]), w_refs[0])
    for t, here in enumerate(tiles):
        if t + 1 < len(tiles):
            build_laplacian(weight_tables(cell_ref, frac_ref, tiles[t + 1]), w_refs[(t + 1) % 2])
        lapt_ref[:, here] = mm(chosen, w_refs[t % 2][...]).astype(BF16)


def eval_kernel(turned_ref, cell_ref, frac_ref, val_ref, lap_ref, *w_refs, first):
    electrons = val_ref.shape[1]

    def build(t):
        tables = weight_tables(cell_ref, frac_ref, slice(first + t * TILE, first + (t + 1) * TILE))
        build_value(tables, w_refs[2 * (t % 2)])
        build_laplacian(tables, w_refs[2 * (t % 2) + 1])

    build(0)
    for t in range(electrons // TILE):
        if (t + 1) * TILE < electrons:
            build(t + 1)
        here = slice(t * TILE, (t + 1) * TILE)
        val_ref[:, here] = mm(turned_ref[...], w_refs[2 * (t % 2)][...]).astype(BF16)
        lap_ref[:, here] = mm(turned_ref[...], w_refs[2 * (t % 2) + 1][...]).astype(BF16)


def place(z_count):
    core, z, plane = lax.axis_index("core"), lax.axis_index("z"), lax.axis_index("xh")
    return plane, [lax.rem(z + dz, z_count) for dz in (0, z_count - 1, 1, 2)], core


def owners(z_count):
    plane, along, core = place(z_count)
    return [(p * z_count + z) * 2 + c for c in (core, 1 - core) for p in (plane, 1 - plane) for z in along]


def inverse_times(z_count, inv_refs, right, out_ref, size):
    blocks = owners(z_count)
    first = 0
    for ref in inv_refs:
        value = mm_nt(ref[...], right).astype(out_ref.dtype)
        count = ref.shape[0] // size
        for j, block in enumerate(blocks[first:first + count]):
            start = pl.multiple_of(block * size, size)
            out_ref[pl.ds(start, size), :] = value[j * size:(j + 1) * size]
        first += count


def ratio_kernel(*refs, parts, z_count, slots, size):
    inv_refs, val_refs = refs[:parts], refs[parts:-3]
    slot_ref, rows_ref, ratio_ref = refs[-3:]
    val = jnp.concatenate([ref[...] for ref in val_refs], axis=1)
    inverse_times(z_count, inv_refs, val, ratio_ref, size)
    ratio = ratio_ref[...]
    slot = slot_ref[...]
    blocks = owners(z_count)
    for j in range(0, len(blocks), 2):
        ids = lax.broadcasted_iota(jnp.int32, (slots, slot.shape[1]), 0)
        pick = jnp.concatenate([(ids + block * slots == slot).astype(F32) for block in blocks[j:j + 2]], axis=0)
        rows_ref[j * slots:(j + 2) * slots, :] = mm(pick.astype(BF16), ratio).astype(BF16)


def coupled(rows_ref, pieces):
    total = None
    for first, ref in pieces:
        term = mm_tn(rows_ref[first:first + ref.shape[0], :], ref[...])
        total = term if total is None else total + term
    return total


def couple_kernel(energy_ref, weight_ref, near_own_ref, near_other_ref, rows_ref, val_a, val_b, lap_a, lap_b, mixed_ref):
    half = rows_ref.shape[0] // 2
    total = coupled(rows_ref, [(0, near_own_ref), (half, near_other_ref)])
    val = jnp.concatenate([val_a[...], val_b[...]], axis=1).astype(F32)
    lap = jnp.concatenate([lap_a[...], lap_b[...]], axis=1).astype(F32)
    mixed_ref[...] = energy_ref[...] * val - 0.5 * (lap - total)


def finish_kernel(weight_ref, mixed_ref, rows_ref, far_own_ref, far_other_ref, *refs, z_count, size):
    inv_refs, out_ref = refs[:-1], refs[-1]
    half = rows_ref.shape[0] // 2
    near = half - far_own_ref.shape[0]
    total = coupled(rows_ref, [(near, far_own_ref), (half + near, far_other_ref)])
    mixed = (weight_ref[...] * (mixed_ref[...] + 0.5 * total)).astype(BF16)
    inverse_times(z_count, inv_refs, mixed, out_ref, size)


VMEM = pl.BlockSpec(memory_space=pltpu.VMEM)
HBM = pl.BlockSpec(memory_space=pltpu.HBM)


def ring_swap(piece):
    return lax.ppermute(piece, "xh", [(0, 1), (1, 0)])


def ring_pass(piece, shift):
    count = lax.axis_size("z")
    return lax.ppermute(piece, "z", [(i, (i + shift) % count) for i in range(count)])


def core_swap(piece):
    return lax.ppermute(piece, "core", [(0, 1), (1, 0)])


def gradient(coefficients, inverse, cell_index, fraction, energies, weights, occupied):
    cells, width = coefficients.shape
    _, rows, electrons = inverse.shape
    z_count = lax.axis_size("z")
    shards = 2 * z_count * 2
    slots = 3 * electrons // (2 * shards)

    along_z = (1, -1, 2)
    out = lambda *shape_dtype: jax.ShapeDtypeStruct(*shape_dtype)
    halves = 2
    part = electrons // halves

    def params(mib):
        return pltpu.CompilerParams(vmem_limit_bytes=mib * 1024 * 1024)

    def cost(products):
        return pl.CostEstimate(flops=2 * products, bytes_accessed=2 * cells * width, transcendentals=0)

    def evaluate(h):
        return pl.pallas_call(
            functools.partial(eval_kernel, first=h * part),
            out_shape=[out((width, part), BF16)] * 2,
            in_specs=[VMEM] * 3,
            out_specs=[VMEM] * 2,
            scratch_shapes=[pltpu.VMEM((cells, TILE), BF16)] * 4,
            compiler_params=params(32),
            cost_estimate=cost(2 * part * cells * width),
            name="evaluate",
        )(turned, cell_index, fraction)

    cell_index, fraction = jnp.transpose(cell_index, (1, 0, 2)), jnp.transpose(fraction, (1, 0, 2))
    mine = inverse.reshape(rows, electrons)

    inv_pieces = [mine]
    for shift in along_z:
        inv_pieces.append(ring_pass(mine, shift))
    inv_plane = jnp.concatenate(inv_pieces, axis=0)
    inv_far = ring_swap(inv_plane)
    inv_plane_other = core_swap(inv_plane)
    inv_far_other = core_swap(inv_far)
    inv_all = [inv_plane, inv_far, inv_plane_other, inv_far_other]

    turned = pl.pallas_call(
        turn_kernel,
        out_shape=out((width, cells), BF16),
        in_specs=[HBM],
        out_specs=VMEM,
        scratch_shapes=[pltpu.VMEM((cells, width), BF16), pltpu.SemaphoreType.DMA((8,))],
        compiler_params=params(50),
        cost_estimate=cost(cells * width * 64),
        name="turn",
    )(coefficients)
    lapt_mine, slot = pl.pallas_call(
        functools.partial(early_kernel, shards=shards),
        out_shape=[out((slots, electrons), BF16), out((1, electrons), jnp.int32)],
        in_specs=[VMEM] * 4,
        out_specs=[VMEM] * 2,
        scratch_shapes=[pltpu.VMEM((cells, TILE), BF16)] * 2,
        compiler_params=params(32),
        cost_estimate=cost(slots * cells * electrons),
        name="early",
    )(turned, cell_index, fraction, occupied.reshape(1, electrons))
    val_a, lap_a = evaluate(0)
    val_b, lap_b = evaluate(1)

    lapt_far = ring_swap(lapt_mine)
    near, far = [lapt_mine], []
    for shift in along_z:
        near.append(ring_pass(lapt_mine, shift))
    near.append(lapt_far)
    for shift in along_z:
        far.append(ring_pass(lapt_far, shift))
    near = jnp.concatenate(near, axis=0)
    far = jnp.concatenate(far, axis=0)
    near_other = core_swap(near)
    far_other = core_swap(far)
    total = shards * slots

    ratio_rows = pl.pallas_call(
        functools.partial(ratio_kernel, parts=len(inv_all), z_count=z_count, slots=slots, size=rows),
        out_shape=out((total, width), BF16),
        in_specs=[VMEM] * (len(inv_all) + 3),
        out_specs=VMEM,
        scratch_shapes=[pltpu.VMEM((electrons, width), BF16)],
        compiler_params=params(24),
        cost_estimate=cost(3 * electrons * electrons * width),
        name="ratio",
    )(*inv_all, val_a, val_b, slot)

    energy, weight = energies.reshape(1, 1), weights.reshape(1, 1)
    mixed = pl.pallas_call(
        couple_kernel,
        out_shape=out((width, electrons), F32),
        in_specs=[VMEM] * 9,
        out_specs=VMEM,
        compiler_params=params(24),
        cost_estimate=cost(electrons * electrons * width),
        name="couple",
    )(energy, weight, near, near_other, ratio_rows, val_a, val_b, lap_a, lap_b)

    partial = pl.pallas_call(
        functools.partial(finish_kernel, z_count=z_count, size=rows),
        out_shape=out((electrons, width), BF16),
        in_specs=[VMEM] * (5 + len(inv_all)),
        out_specs=VMEM,
        compiler_params=params(24),
        cost_estimate=cost(electrons * electrons * width),
        name="finish",
    )(weight, mixed, ratio_rows, far, far_other, *inv_all)

    walkers = ("y", "xl")
    count = lax.axis_size(walkers)
    blocks = lax.all_to_all(partial.reshape(count, electrons // count, width), walkers, 0, 0, tiled=True)
    return jnp.sum(blocks.astype(F32), axis=0)


def solution(mesh):
    fine = Mesh(mesh.devices.reshape(4, 2, 2, 4, 2), ("y", "xl", "xh", "z", "core"))
    walk, orb = ("y", "xl"), ("xh", "z", "core")
    in_specs = (
        P(None, orb),
        P(walk, orb, None),
        P(walk, None, None),
        P(walk, None, None),
        P(walk),
        P(walk),
        P(),
    )
    return jax.shard_map(gradient, mesh=fine, in_specs=in_specs, out_specs=P(walk, orb), check_vma=False)
```

```python
import functools

import jax
import jax.numpy as jnp
from jax import lax
from jax.experimental import pallas as pl
from jax.experimental.pallas import tpu as pltpu
from jax.sharding import Mesh
from jax.sharding import PartitionSpec as P


GRID = 16
PLANE = GRID * GRID
TILE = 256
BF16 = jnp.bfloat16
F32 = jnp.float32


def mm(left, right):
    return jnp.dot(left, right, preferred_element_type=F32)


def mm_nt(left, right):
    return lax.dot_general(left, right, (((1,), (1,)), ((), ())), preferred_element_type=F32)


def mm_tn(left, right):
    return lax.dot_general(left, right, (((0,), (0,)), ((), ())), preferred_element_type=F32)


def dense_rows(cell, frac):
    remain = 1.0 - frac
    square = frac * frac
    cubed = square * frac
    sixth = 1.0 / 6.0
    values = [
        remain * remain * remain * sixth,
        (3.0 * cubed - 6.0 * square + 4.0) * sixth,
        (-3.0 * cubed + 3.0 * square + 3.0 * frac + 1.0) * sixth,
        cubed * sixth,
    ]
    curves = [remain, 3.0 * frac - 2.0, 1.0 - 3.0 * frac, frac]
    line = lax.broadcasted_iota(jnp.int32, (GRID, cell.shape[1]), 0)
    tap = (line - cell + (GRID + 1)) & (GRID - 1)
    value = jnp.zeros((GRID, cell.shape[1]), F32)
    curve = jnp.zeros((GRID, cell.shape[1]), F32)
    for a in range(4):
        value = jnp.where(tap == a, values[a], value)
        curve = jnp.where(tap == a, curves[a], curve)
    return value, curve


def slot_tables(me, occ, shards, width, slots):
    owner = lax.broadcasted_iota(jnp.int32, (shards, occ.shape[1]), 0) == lax.div(occ, width)
    count = owner.astype(jnp.int32)
    lane = lax.broadcasted_iota(jnp.int32, count.shape, 1)
    step = 1
    while step < occ.shape[1]:
        count = count + jnp.where(lane >= step, pltpu.roll(count, step, 1), 0)
        step *= 2
    rank = jnp.sum(jnp.where(owner, count - 1, 0), axis=0, keepdims=True)
    slot = lax.div(occ, width) * slots + rank
    placed = lax.broadcasted_iota(jnp.int32, (slots, occ.shape[1]), 0) == slot - me * slots
    column = lax.broadcasted_iota(jnp.int32, (width, occ.shape[1]), 0) == occ - me * width
    picker = mm_nt(placed.astype(F32).astype(BF16), column.astype(F32).astype(BF16)).astype(BF16)
    return slot, picker


def expand(rows, weights):
    return jnp.concatenate([rows[g:g + 1, :] * weights for g in range(GRID)], axis=0)


def turn_kernel(coef_hbm, turned_ref, coef_ref, sems):
    pieces = sems.shape[0]
    rows = coef_ref.shape[0] // pieces
    copies = [
        pltpu.make_async_copy(coef_hbm.at[pl.ds(k * rows, rows)], coef_ref.at[pl.ds(k * rows, rows)], sems.at[k])
        for k in range(pieces)
    ]
    for copy in copies:
        copy.start()
    for k, copy in enumerate(copies):
        copy.wait()
        for first in range(k * rows, (k + 1) * rows, PLANE):
            turned_ref[:, first:first + PLANE] = jnp.transpose(coef_ref[first:first + PLANE, :])


def weight_tables(cell_ref, frac_ref, here):
    tables = [dense_rows(cell_ref[k, :, here], frac_ref[k, :, here]) for k in range(3)]
    (vx, cx), (vy, cy), (vz, cz) = tables
    return vx, cx, expand(vy, vz), expand(cy, vz) + expand(vy, cz)


def build_laplacian(tables, w_ref):
    vx, cx, value, curve = tables
    for g in range(GRID):
        w_ref[g * PLANE:(g + 1) * PLANE, :] = (cx[g:g + 1, :] * value + vx[g:g + 1, :] * curve).astype(BF16)


def build_value(tables, w_ref):
    vx, _, value, _ = tables
    for g in range(GRID):
        w_ref[g * PLANE:(g + 1) * PLANE, :] = (vx[g:g + 1, :] * value).astype(BF16)


def early_kernel(turned_ref, cell_ref, frac_ref, occ_ref, lapt_ref, slot_ref, *w_refs, shards):
    slots, electrons = lapt_ref.shape
    plane, along, core = place(shards // 4)
    me = (plane * (shards // 4) + along[0]) * 2 + core
    slot, picker = slot_tables(me, occ_ref[...], shards, turned_ref.shape[0], slots)
    slot_ref[...] = slot
    chosen = mm(picker, turned_ref[...]).astype(BF16)

    def build(t):
        vx, cx, value, curve = weight_tables(cell_ref, frac_ref, slice(t * TILE, (t + 1) * TILE))
        value = value.astype(BF16).reshape(GRID, GRID, TILE)
        curve = curve.astype(BF16).reshape(GRID, GRID, TILE)
        for g in range(GRID):
            x_value = jnp.broadcast_to(vx[g:g + 1, :], (GRID, TILE)).astype(BF16)[None]
            x_curve = jnp.broadcast_to(cx[g:g + 1, :], (GRID, TILE)).astype(BF16)[None]
            w_refs[t % 2][g * PLANE:(g + 1) * PLANE, :] = (x_curve * value + x_value * curve).reshape(PLANE, TILE)

    build(0)
    for t in range(electrons // TILE):
        if (t + 1) * TILE < electrons:
            build(t + 1)
        lapt_ref[:, t * TILE:(t + 1) * TILE] = mm(chosen, w_refs[t % 2][...]).astype(BF16)


def eval_kernel(turned_ref, cell_ref, frac_ref, val_ref, lap_ref, *w_refs, first):
    electrons = val_ref.shape[1]

    def build(t):
        tables = weight_tables(cell_ref, frac_ref, slice(first + t * TILE, first + (t + 1) * TILE))
        build_value(tables, w_refs[2 * (t % 2)])
        build_laplacian(tables, w_refs[2 * (t % 2) + 1])

    build(0)
    for t in range(electrons // TILE):
        if (t + 1) * TILE < electrons:
            build(t + 1)
        here = slice(t * TILE, (t + 1) * TILE)
        val_ref[:, here] = mm(turned_ref[...], w_refs[2 * (t % 2)][...]).astype(BF16)
        lap_ref[:, here] = mm(turned_ref[...], w_refs[2 * (t % 2) + 1][...]).astype(BF16)


def place(z_count):
    core, z, plane = lax.axis_index("core"), lax.axis_index("z"), lax.axis_index("xh")
    return plane, [lax.rem(z + dz, z_count) for dz in (0, z_count - 1, 1, 2)], core


def owners(z_count):
    plane, along, core = place(z_count)
    return [(p * z_count + z) * 2 + c for c in (core, 1 - core) for p in (plane, 1 - plane) for z in along]


def inverse_times(z_count, inv_refs, right, out_ref, size):
    blocks = owners(z_count)
    first = 0
    for ref in inv_refs:
        value = mm_nt(ref[...], right).astype(out_ref.dtype)
        count = ref.shape[0] // size
        for j, block in enumerate(blocks[first:first + count]):
            start = pl.multiple_of(block * size, size)
            out_ref[pl.ds(start, size), :] = value[j * size:(j + 1) * size]
        first += count


def ratio_kernel(*refs, parts, z_count, slots, size):
    inv_refs, val_refs = refs[:parts], refs[parts:-3]
    slot_ref, rows_ref, ratio_ref = refs[-3:]
    val = jnp.concatenate([ref[...] for ref in val_refs], axis=1)
    inverse_times(z_count, inv_refs, val, ratio_ref, size)
    ratio = ratio_ref[...]
    slot = slot_ref[...]
    blocks = owners(z_count)
    for j in range(0, len(blocks), 2):
        ids = lax.broadcasted_iota(jnp.int32, (slots, slot.shape[1]), 0)
        pick = jnp.concatenate([(ids + block * slots == slot).astype(F32) for block in blocks[j:j + 2]], axis=0)
        rows_ref[j * slots:(j + 2) * slots, :] = mm(pick.astype(BF16), ratio).astype(BF16)


def coupled(rows_ref, pieces):
    total = None
    for first, ref in pieces:
        term = mm_tn(rows_ref[first:first + ref.shape[0], :], ref[...])
        total = term if total is None else total + term
    return total


def finish_kernel(energy_ref, weight_ref, near_own_ref, far_own_ref, near_other_ref, far_other_ref, rows_ref,
                  val_a, val_b, lap_a, lap_b, *refs, z_count, size):
    inv_refs, out_ref = refs[:-1], refs[-1]
    half = rows_ref.shape[0] // 2
    near = near_own_ref.shape[0]
    total = coupled(rows_ref, [
        (0, near_own_ref), (near, far_own_ref), (half, near_other_ref), (half + near, far_other_ref)
    ])
    val = jnp.concatenate([val_a[...], val_b[...]], axis=1).astype(F32)
    lap = jnp.concatenate([lap_a[...], lap_b[...]], axis=1).astype(F32)
    mixed = (weight_ref[...] * (energy_ref[...] * val - 0.5 * (lap - total))).astype(BF16)
    inverse_times(z_count, inv_refs, mixed, out_ref, size)


VMEM = pl.BlockSpec(memory_space=pltpu.VMEM)
HBM = pl.BlockSpec(memory_space=pltpu.HBM)


def ring_swap(piece):
    return lax.ppermute(piece, "xh", [(0, 1), (1, 0)])


def ring_pass(piece, shift):
    count = lax.axis_size("z")
    return lax.ppermute(piece, "z", [(i, (i + shift) % count) for i in range(count)])


def core_swap(piece):
    return lax.ppermute(piece, "core", [(0, 1), (1, 0)])


def gradient(coefficients, inverse, cell_index, fraction, energies, weights, occupied):
    cells, width = coefficients.shape
    _, rows, electrons = inverse.shape
    z_count = lax.axis_size("z")
    shards = 2 * z_count * 2
    slots = 3 * electrons // (2 * shards)

    along_z = (1, -1, 2)
    out = lambda *shape_dtype: jax.ShapeDtypeStruct(*shape_dtype)
    halves = 2
    part = electrons // halves

    def params(mib):
        return pltpu.CompilerParams(vmem_limit_bytes=mib * 1024 * 1024)

    def cost(products):
        return pl.CostEstimate(flops=2 * products, bytes_accessed=2 * cells * width, transcendentals=0)

    def evaluate(h):
        return pl.pallas_call(
            functools.partial(eval_kernel, first=h * part),
            out_shape=[out((width, part), BF16)] * 2,
            in_specs=[VMEM] * 3,
            out_specs=[VMEM] * 2,
            scratch_shapes=[pltpu.VMEM((cells, TILE), BF16)] * 4,
            compiler_params=params(32),
            cost_estimate=cost(2 * part * cells * width),
            name="evaluate",
        )(turned, cell_index, fraction)

    cell_index, fraction = jnp.transpose(cell_index, (1, 0, 2)), jnp.transpose(fraction, (1, 0, 2))
    mine = inverse.reshape(rows, electrons)

    inv_pieces = []
    for shift in along_z:
        inv_pieces.append(ring_pass(mine, shift))
    inv_far_mine = ring_swap(mine)
    inv_rest = jnp.concatenate(inv_pieces, axis=0)
    inv_far_rest = ring_swap(inv_rest)
    inv_plane = jnp.concatenate([mine, inv_rest], axis=0)
    inv_far = jnp.concatenate([inv_far_mine, inv_far_rest], axis=0)
    inv_plane_other = core_swap(inv_plane)
    inv_far_other = core_swap(inv_far)
    inv_all = [inv_plane, inv_far, inv_plane_other, inv_far_other]

    turned = pl.pallas_call(
        turn_kernel,
        out_shape=out((width, cells), BF16),
        in_specs=[HBM],
        out_specs=VMEM,
        scratch_shapes=[pltpu.VMEM((cells, width), BF16), pltpu.SemaphoreType.DMA((8,))],
        compiler_params=params(50),
        cost_estimate=cost(cells * width * 64),
        name="turn",
    )(coefficients)
    lapt_mine, slot = pl.pallas_call(
        functools.partial(early_kernel, shards=shards),
        out_shape=[out((slots, electrons), BF16), out((1, electrons), jnp.int32)],
        in_specs=[VMEM] * 4,
        out_specs=[VMEM] * 2,
        scratch_shapes=[pltpu.VMEM((cells, TILE), BF16)] * 2,
        compiler_params=params(32),
        cost_estimate=cost(slots * cells * electrons),
        name="early",
    )(turned, cell_index, fraction, occupied.reshape(1, electrons))
    val_a, lap_a = evaluate(0)
    val_b, lap_b = evaluate(1)

    lapt_far = ring_swap(lapt_mine)
    near, far = [lapt_mine], []
    for shift in along_z:
        near.append(ring_pass(lapt_mine, shift))
    near.append(lapt_far)
    for shift in along_z:
        far.append(ring_pass(lapt_far, shift))
    near = jnp.concatenate(near, axis=0)
    far = jnp.concatenate(far, axis=0)
    near_other = core_swap(near)
    far_other = core_swap(far)
    total = shards * slots

    ratio_rows = pl.pallas_call(
        functools.partial(ratio_kernel, parts=len(inv_all), z_count=z_count, slots=slots, size=rows),
        out_shape=out((total, width), BF16),
        in_specs=[VMEM] * (len(inv_all) + 3),
        out_specs=VMEM,
        scratch_shapes=[pltpu.VMEM((electrons, width), BF16)],
        compiler_params=params(24),
        cost_estimate=cost(3 * electrons * electrons * width),
        name="ratio",
    )(*inv_all, val_a, val_b, slot)

    energy, weight = energies.reshape(1, 1), weights.reshape(1, 1)
    partial = pl.pallas_call(
        functools.partial(finish_kernel, z_count=z_count, size=rows),
        out_shape=out((electrons, width), BF16),
        in_specs=[VMEM] * (11 + len(inv_all)),
        out_specs=VMEM,
        compiler_params=params(24),
        cost_estimate=cost(3 * electrons * electrons * width),
        name="finish",
    )(energy, weight, near, far, near_other, far_other, ratio_rows, val_a, val_b, lap_a, lap_b, *inv_all)

    walkers = ("y", "xl")
    count = lax.axis_size(walkers)
    blocks = lax.all_to_all(partial.reshape(count, electrons // count, width), walkers, 0, 0, tiled=True)
    return jnp.sum(blocks.astype(F32), axis=0)


def solution(mesh):
    fine = Mesh(mesh.devices.reshape(4, 2, 2, 4, 2), ("y", "xl", "xh", "z", "core"))
    walk, orb = ("y", "xl"), ("xh", "z", "core")
    in_specs = (
        P(None, orb),
        P(walk, orb, None),
        P(walk, None, None),
        P(walk, None, None),
        P(walk),
        P(walk),
        P(),
    )
    return jax.shard_map(gradient, mesh=fine, in_specs=in_specs, out_specs=P(walk, orb), check_vma=False)
```

```python
import functools

import jax
import jax.numpy as jnp
from jax import lax
from jax.experimental import pallas as pl
from jax.experimental.pallas import tpu as pltpu
from jax.sharding import Mesh
from jax.sharding import PartitionSpec as P


GRID = 16
PLANE = GRID * GRID
TILE = 256
BF16 = jnp.bfloat16
F32 = jnp.float32


def mm(left, right):
    return jnp.dot(left, right, preferred_element_type=F32)


def mm_nt(left, right):
    return lax.dot_general(left, right, (((1,), (1,)), ((), ())), preferred_element_type=F32)


def mm_tn(left, right):
    return lax.dot_general(left, right, (((0,), (0,)), ((), ())), preferred_element_type=F32)


def dense_rows(cell, frac):
    remain = 1.0 - frac
    square = frac * frac
    cubed = square * frac
    sixth = 1.0 / 6.0
    values = [
        remain * remain * remain * sixth,
        (3.0 * cubed - 6.0 * square + 4.0) * sixth,
        (-3.0 * cubed + 3.0 * square + 3.0 * frac + 1.0) * sixth,
        cubed * sixth,
    ]
    curves = [remain, 3.0 * frac - 2.0, 1.0 - 3.0 * frac, frac]
    line = lax.broadcasted_iota(jnp.int32, (GRID, cell.shape[1]), 0)
    tap = (line - cell + (GRID + 1)) & (GRID - 1)
    value = jnp.zeros((GRID, cell.shape[1]), F32)
    curve = jnp.zeros((GRID, cell.shape[1]), F32)
    for a in range(4):
        value = jnp.where(tap == a, values[a], value)
        curve = jnp.where(tap == a, curves[a], curve)
    return value, curve


def slot_tables(me, occ, shards, width, slots):
    owner = lax.broadcasted_iota(jnp.int32, (shards, occ.shape[1]), 0) == lax.div(occ, width)
    count = owner.astype(jnp.int32)
    lane = lax.broadcasted_iota(jnp.int32, count.shape, 1)
    step = 1
    while step < occ.shape[1]:
        count = count + jnp.where(lane >= step, pltpu.roll(count, step, 1), 0)
        step *= 2
    rank = jnp.sum(jnp.where(owner, count - 1, 0), axis=0, keepdims=True)
    slot = lax.div(occ, width) * slots + rank
    placed = lax.broadcasted_iota(jnp.int32, (slots, occ.shape[1]), 0) == slot - me * slots
    column = lax.broadcasted_iota(jnp.int32, (width, occ.shape[1]), 0) == occ - me * width
    picker = mm_nt(placed.astype(F32).astype(BF16), column.astype(F32).astype(BF16)).astype(BF16)
    return slot, picker


def expand(rows, weights):
    return jnp.concatenate([rows[g:g + 1, :] * weights for g in range(GRID)], axis=0)


def turn_kernel(coef_hbm, turned_ref, coef_ref, sems):
    pieces = sems.shape[0]
    rows = coef_ref.shape[0] // pieces
    copies = [
        pltpu.make_async_copy(coef_hbm.at[pl.ds(k * rows, rows)], coef_ref.at[pl.ds(k * rows, rows)], sems.at[k])
        for k in range(pieces)
    ]
    for copy in copies:
        copy.start()
    for k, copy in enumerate(copies):
        copy.wait()
        for first in range(k * rows, (k + 1) * rows, PLANE):
            turned_ref[:, first:first + PLANE] = jnp.transpose(coef_ref[first:first + PLANE, :])


def weight_tables(cell_ref, frac_ref, here):
    tables = [dense_rows(cell_ref[k, :, here], frac_ref[k, :, here]) for k in range(3)]
    (vx, cx), (vy, cy), (vz, cz) = tables
    return vx, cx, expand(vy, vz), expand(cy, vz) + expand(vy, cz)


def build_laplacian(tables, w_ref):
    vx, cx, value, curve = tables
    for g in range(GRID):
        w_ref[g * PLANE:(g + 1) * PLANE, :] = (cx[g:g + 1, :] * value + vx[g:g + 1, :] * curve).astype(BF16)


def build_value(tables, w_ref):
    vx, _, value, _ = tables
    for g in range(GRID):
        w_ref[g * PLANE:(g + 1) * PLANE, :] = (vx[g:g + 1, :] * value).astype(BF16)


def early_kernel(turned_ref, cell_ref, frac_ref, occ_ref, lapt_ref, slot_ref, *w_refs, shards):
    slots, electrons = lapt_ref.shape
    plane, z, core = place()
    me = (plane * (shards // 4) + z) * 2 + core
    slot, picker = slot_tables(me, occ_ref[...], shards, turned_ref.shape[0], slots)
    slot_ref[...] = slot
    chosen = mm(picker, turned_ref[...]).astype(BF16)

    def build(t):
        vx, cx, value, curve = weight_tables(cell_ref, frac_ref, slice(t * TILE, (t + 1) * TILE))
        value = value.astype(BF16).reshape(GRID, GRID, TILE)
        curve = curve.astype(BF16).reshape(GRID, GRID, TILE)
        for g in range(GRID):
            x_value = jnp.broadcast_to(vx[g:g + 1, :], (GRID, TILE)).astype(BF16)[None]
            x_curve = jnp.broadcast_to(cx[g:g + 1, :], (GRID, TILE)).astype(BF16)[None]
            w_refs[t % 2][g * PLANE:(g + 1) * PLANE, :] = (x_curve * value + x_value * curve).reshape(PLANE, TILE)

    build(0)
    for t in range(electrons // TILE):
        if (t + 1) * TILE < electrons:
            build(t + 1)
        lapt_ref[:, t * TILE:(t + 1) * TILE] = mm(chosen, w_refs[t % 2][...]).astype(BF16)


def eval_kernel(turned_ref, cell_ref, frac_ref, val_ref, lap_ref, *w_refs, first):
    electrons = val_ref.shape[1]

    def build(t):
        tables = weight_tables(cell_ref, frac_ref, slice(first + t * TILE, first + (t + 1) * TILE))
        build_value(tables, w_refs[2 * (t % 2)])
        build_laplacian(tables, w_refs[2 * (t % 2) + 1])

    build(0)
    for t in range(electrons // TILE):
        if (t + 1) * TILE < electrons:
            build(t + 1)
        here = slice(t * TILE, (t + 1) * TILE)
        val_ref[:, here] = mm(turned_ref[...], w_refs[2 * (t % 2)][...]).astype(BF16)
        lap_ref[:, here] = mm(turned_ref[...], w_refs[2 * (t % 2) + 1][...]).astype(BF16)


def place():
    return lax.axis_index("xh"), lax.axis_index("z"), lax.axis_index("core")


def owners(z_count, along):
    plane, _, core = place()
    return [(p * z_count + z) * 2 + c for c in (core, 1 - core) for p in (plane, 1 - plane) for z in along]


def inverse_owners(z_count):
    z = place()[1]
    return owners(z_count, [z ^ k for k in (0, 1, 3, 2)])


def slot_owners(z_count):
    z = place()[1]
    return owners(z_count, [lax.rem(z + k, z_count) for k in (0, z_count - 1, 1, 2)])


def inverse_times(z_count, inv_refs, right, out_ref, size):
    blocks = inverse_owners(z_count)
    first = 0
    for ref in inv_refs:
        value = mm_nt(ref[...], right).astype(out_ref.dtype)
        count = ref.shape[0] // size
        for j, block in enumerate(blocks[first:first + count]):
            start = pl.multiple_of(block * size, size)
            out_ref[pl.ds(start, size), :] = value[j * size:(j + 1) * size]
        first += count


def ratio_kernel(*refs, parts, z_count, slots, size):
    inv_refs, val_refs = refs[:parts], refs[parts:-3]
    slot_ref, rows_ref, ratio_ref = refs[-3:]
    val = jnp.concatenate([ref[...] for ref in val_refs], axis=1)
    inverse_times(z_count, inv_refs, val, ratio_ref, size)
    ratio = ratio_ref[...]
    slot = slot_ref[...]
    blocks = slot_owners(z_count)
    for j in range(0, len(blocks), 2):
        ids = lax.broadcasted_iota(jnp.int32, (slots, slot.shape[1]), 0)
        pick = jnp.concatenate([(ids + block * slots == slot).astype(F32) for block in blocks[j:j + 2]], axis=0)
        rows_ref[j * slots:(j + 2) * slots, :] = mm(pick.astype(BF16), ratio).astype(BF16)


def coupled(rows_ref, pieces):
    total = None
    for first, ref in pieces:
        term = mm_tn(rows_ref[first:first + ref.shape[0], :], ref[...])
        total = term if total is None else total + term
    return total


def finish_kernel(energy_ref, weight_ref, near_own_ref, far_own_ref, near_other_ref, far_other_ref, rows_ref,
                  val_a, val_b, lap_a, lap_b, *refs, z_count, size):
    inv_refs, out_ref = refs[:-1], refs[-1]
    half = rows_ref.shape[0] // 2
    near = near_own_ref.shape[0]
    total = coupled(rows_ref, [
        (0, near_own_ref), (near, far_own_ref), (half, near_other_ref), (half + near, far_other_ref)
    ])
    val = jnp.concatenate([val_a[...], val_b[...]], axis=1).astype(F32)
    lap = jnp.concatenate([lap_a[...], lap_b[...]], axis=1).astype(F32)
    mixed = (weight_ref[...] * (energy_ref[...] * val - 0.5 * (lap - total))).astype(BF16)
    inverse_times(z_count, inv_refs, mixed, out_ref, size)


VMEM = pl.BlockSpec(memory_space=pltpu.VMEM)
HBM = pl.BlockSpec(memory_space=pltpu.HBM)


def ring_swap(piece):
    return lax.ppermute(piece, "xh", [(0, 1), (1, 0)])


def ring_pass(piece, shift):
    count = lax.axis_size("z")
    return lax.ppermute(piece, "z", [(i, (i + shift) % count) for i in range(count)])


def ring_trade(piece, bits):
    return lax.ppermute(piece, "z", [(i, i ^ bits) for i in range(lax.axis_size("z"))])


def core_swap(piece):
    return lax.ppermute(piece, "core", [(0, 1), (1, 0)])


def gradient(coefficients, inverse, cell_index, fraction, energies, weights, occupied):
    cells, width = coefficients.shape
    _, rows, electrons = inverse.shape
    z_count = lax.axis_size("z")
    shards = 2 * z_count * 2
    slots = 3 * electrons // (2 * shards)

    along_z = (1, -1, 2)
    out = lambda *shape_dtype: jax.ShapeDtypeStruct(*shape_dtype)
    halves = 2
    part = electrons // halves

    def params(mib):
        return pltpu.CompilerParams(vmem_limit_bytes=mib * 1024 * 1024)

    def cost(products):
        return pl.CostEstimate(flops=2 * products, bytes_accessed=2 * cells * width, transcendentals=0)

    def evaluate(h):
        return pl.pallas_call(
            functools.partial(eval_kernel, first=h * part),
            out_shape=[out((width, part), BF16)] * 2,
            in_specs=[VMEM] * 3,
            out_specs=[VMEM] * 2,
            scratch_shapes=[pltpu.VMEM((cells, TILE), BF16)] * 4,
            compiler_params=params(32),
            cost_estimate=cost(2 * part * cells * width),
            name="evaluate",
        )(turned, cell_index, fraction)

    cell_index, fraction = jnp.transpose(cell_index, (1, 0, 2)), jnp.transpose(fraction, (1, 0, 2))
    mine = inverse.reshape(rows, electrons)

    inv_pair = jnp.concatenate([mine, ring_trade(mine, 1)], axis=0)
    inv_plane = jnp.concatenate([inv_pair, ring_trade(inv_pair, 3)], axis=0)
    inv_far = ring_swap(inv_plane)
    inv_plane_other = core_swap(inv_plane)
    inv_far_other = core_swap(inv_far)
    inv_all = [inv_plane, inv_far, inv_plane_other, inv_far_other]

    turned = pl.pallas_call(
        turn_kernel,
        out_shape=out((width, cells), BF16),
        in_specs=[HBM],
        out_specs=VMEM,
        scratch_shapes=[pltpu.VMEM((cells, width), BF16), pltpu.SemaphoreType.DMA((8,))],
        compiler_params=params(50),
        cost_estimate=cost(cells * width * 64),
        name="turn",
    )(coefficients)
    lapt_mine, slot = pl.pallas_call(
        functools.partial(early_kernel, shards=shards),
        out_shape=[out((slots, electrons), BF16), out((1, electrons), jnp.int32)],
        in_specs=[VMEM] * 4,
        out_specs=[VMEM] * 2,
        scratch_shapes=[pltpu.VMEM((cells, TILE), BF16)] * 2,
        compiler_params=params(32),
        cost_estimate=cost(slots * cells * electrons),
        name="early",
    )(turned, cell_index, fraction, occupied.reshape(1, electrons))
    val_a, lap_a = evaluate(0)
    val_b, lap_b = evaluate(1)

    lapt_far = ring_swap(lapt_mine)
    near, far = [lapt_mine], []
    for shift in along_z:
        near.append(ring_pass(lapt_mine, shift))
    near.append(lapt_far)
    for shift in along_z:
        far.append(ring_pass(lapt_far, shift))
    near = jnp.concatenate(near, axis=0)
    far = jnp.concatenate(far, axis=0)
    near_other = core_swap(near)
    far_other = core_swap(far)
    total = shards * slots

    ratio_rows = pl.pallas_call(
        functools.partial(ratio_kernel, parts=len(inv_all), z_count=z_count, slots=slots, size=rows),
        out_shape=out((total, width), BF16),
        in_specs=[VMEM] * (len(inv_all) + 3),
        out_specs=VMEM,
        scratch_shapes=[pltpu.VMEM((electrons, width), BF16)],
        compiler_params=params(24),
        cost_estimate=cost(3 * electrons * electrons * width),
        name="ratio",
    )(*inv_all, val_a, val_b, slot)

    energy, weight = energies.reshape(1, 1), weights.reshape(1, 1)
    partial = pl.pallas_call(
        functools.partial(finish_kernel, z_count=z_count, size=rows),
        out_shape=out((electrons, width), BF16),
        in_specs=[VMEM] * (11 + len(inv_all)),
        out_specs=VMEM,
        compiler_params=params(24),
        cost_estimate=cost(3 * electrons * electrons * width),
        name="finish",
    )(energy, weight, near, far, near_other, far_other, ratio_rows, val_a, val_b, lap_a, lap_b, *inv_all)

    walkers = ("y", "xl")
    count = lax.axis_size(walkers)
    blocks = lax.all_to_all(partial.reshape(count, electrons // count, width), walkers, 0, 0, tiled=True)
    return jnp.sum(blocks.astype(F32), axis=0)


def solution(mesh):
    fine = Mesh(mesh.devices.reshape(4, 2, 2, 4, 2), ("y", "xl", "xh", "z", "core"))
    walk, orb = ("y", "xl"), ("xh", "z", "core")
    in_specs = (
        P(None, orb),
        P(walk, orb, None),
        P(walk, None, None),
        P(walk, None, None),
        P(walk),
        P(walk),
        P(),
    )
    return jax.shard_map(gradient, mesh=fine, in_specs=in_specs, out_specs=P(walk, orb), check_vma=False)
```

```python
import functools

import jax
import jax.numpy as jnp
from jax import lax
from jax.experimental import pallas as pl
from jax.experimental.pallas import tpu as pltpu
from jax.sharding import Mesh
from jax.sharding import PartitionSpec as P


GRID = 16
PLANE = GRID * GRID
TILE = 256
BF16 = jnp.bfloat16
F32 = jnp.float32


def mm(left, right):
    return jnp.dot(left, right, preferred_element_type=F32)


def mm_nt(left, right):
    return lax.dot_general(left, right, (((1,), (1,)), ((), ())), preferred_element_type=F32)


def mm_tn(left, right):
    return lax.dot_general(left, right, (((0,), (0,)), ((), ())), preferred_element_type=F32)


def dense_rows(cell, frac):
    remain = 1.0 - frac
    square = frac * frac
    cubed = square * frac
    sixth = 1.0 / 6.0
    values = [
        remain * remain * remain * sixth,
        (3.0 * cubed - 6.0 * square + 4.0) * sixth,
        (-3.0 * cubed + 3.0 * square + 3.0 * frac + 1.0) * sixth,
        cubed * sixth,
    ]
    curves = [remain, 3.0 * frac - 2.0, 1.0 - 3.0 * frac, frac]
    line = lax.broadcasted_iota(jnp.int32, (GRID, cell.shape[1]), 0)
    tap = (line - cell + (GRID + 1)) & (GRID - 1)
    value = jnp.zeros((GRID, cell.shape[1]), F32)
    curve = jnp.zeros((GRID, cell.shape[1]), F32)
    for a in range(4):
        value = jnp.where(tap == a, values[a], value)
        curve = jnp.where(tap == a, curves[a], curve)
    return value, curve


def slot_tables(me, occ, shards, width, slots):
    owner = lax.broadcasted_iota(jnp.int32, (shards, occ.shape[1]), 0) == lax.div(occ, width)
    count = owner.astype(jnp.int32)
    lane = lax.broadcasted_iota(jnp.int32, count.shape, 1)
    step = 1
    while step < occ.shape[1]:
        count = count + jnp.where(lane >= step, pltpu.roll(count, step, 1), 0)
        step *= 2
    rank = jnp.sum(jnp.where(owner, count - 1, 0), axis=0, keepdims=True)
    slot = lax.div(occ, width) * slots + rank
    placed = lax.broadcasted_iota(jnp.int32, (slots, occ.shape[1]), 0) == slot - me * slots
    column = lax.broadcasted_iota(jnp.int32, (width, occ.shape[1]), 0) == occ - me * width
    picker = mm_nt(placed.astype(F32).astype(BF16), column.astype(F32).astype(BF16)).astype(BF16)
    return slot, picker


def expand(rows, weights):
    return jnp.concatenate([rows[g:g + 1, :] * weights for g in range(GRID)], axis=0)


def turn_kernel(coef_hbm, turned_ref, coef_ref, sems):
    pieces = sems.shape[0]
    rows = coef_ref.shape[0] // pieces
    copies = [
        pltpu.make_async_copy(coef_hbm.at[pl.ds(k * rows, rows)], coef_ref.at[pl.ds(k * rows, rows)], sems.at[k])
        for k in range(pieces)
    ]
    for copy in copies:
        copy.start()
    for k, copy in enumerate(copies):
        copy.wait()
        for first in range(k * rows, (k + 1) * rows, PLANE):
            turned_ref[:, first:first + PLANE] = jnp.transpose(coef_ref[first:first + PLANE, :])


def weight_tables(cell_ref, frac_ref, here):
    tables = [dense_rows(cell_ref[k, :, here], frac_ref[k, :, here]) for k in range(3)]
    (vx, cx), (vy, cy), (vz, cz) = tables
    return vx, cx, expand(vy, vz), expand(cy, vz) + expand(vy, cz)


def build_laplacian(tables, w_ref):
    vx, cx, value, curve = tables
    for g in range(GRID):
        w_ref[g * PLANE:(g + 1) * PLANE, :] = (cx[g:g + 1, :] * value + vx[g:g + 1, :] * curve).astype(BF16)


def build_value(tables, w_ref):
    vx, _, value, _ = tables
    for g in range(GRID):
        w_ref[g * PLANE:(g + 1) * PLANE, :] = (vx[g:g + 1, :] * value).astype(BF16)


def early_kernel(turned_ref, cell_ref, frac_ref, occ_ref, lapt_ref, slot_ref, *w_refs, shards):
    slots, electrons = lapt_ref.shape
    plane, along, core = place(shards // 4)
    me = (plane * (shards // 4) + along[0]) * 2 + core
    slot, picker = slot_tables(me, occ_ref[...], shards, turned_ref.shape[0], slots)
    slot_ref[...] = slot
    chosen = mm(picker, turned_ref[...]).astype(BF16)

    def build(t):
        vx, cx, value, curve = weight_tables(cell_ref, frac_ref, slice(t * TILE, (t + 1) * TILE))
        value = value.astype(BF16).reshape(GRID, GRID, TILE)
        curve = curve.astype(BF16).reshape(GRID, GRID, TILE)
        for g in range(GRID):
            x_value = jnp.broadcast_to(vx[g:g + 1, :], (GRID, TILE)).astype(BF16)[None]
            x_curve = jnp.broadcast_to(cx[g:g + 1, :], (GRID, TILE)).astype(BF16)[None]
            w_refs[t % 2][g * PLANE:(g + 1) * PLANE, :] = (x_curve * value + x_value * curve).reshape(PLANE, TILE)

    build(0)
    for t in range(electrons // TILE):
        if (t + 1) * TILE < electrons:
            build(t + 1)
        lapt_ref[:, t * TILE:(t + 1) * TILE] = mm(chosen, w_refs[t % 2][...]).astype(BF16)


def eval_kernel(turned_ref, cell_ref, frac_ref, val_ref, lap_ref, *w_refs, first):
    electrons = val_ref.shape[1]

    def build(t):
        tables = weight_tables(cell_ref, frac_ref, slice(first + t * TILE, first + (t + 1) * TILE))
        build_value(tables, w_refs[2 * (t % 2)])
        build_laplacian(tables, w_refs[2 * (t % 2) + 1])

    build(0)
    for t in range(electrons // TILE):
        if (t + 1) * TILE < electrons:
            build(t + 1)
        here = slice(t * TILE, (t + 1) * TILE)
        val_ref[:, here] = mm(turned_ref[...], w_refs[2 * (t % 2)][...]).astype(BF16)
        lap_ref[:, here] = mm(turned_ref[...], w_refs[2 * (t % 2) + 1][...]).astype(BF16)


def place(z_count):
    core, z, plane = lax.axis_index("core"), lax.axis_index("z"), lax.axis_index("xh")
    return plane, [lax.rem(z + dz, z_count) for dz in (0, 2, z_count - 1, 1)], core


def owners(z_count):
    plane, along, core = place(z_count)
    return [(p * z_count + z) * 2 + c for c in (core, 1 - core) for p in (plane, 1 - plane) for z in along]


def inverse_times(z_count, inv_refs, right, out_ref, size):
    blocks = owners(z_count)
    first = 0
    for ref in inv_refs:
        value = mm_nt(ref[...], right).astype(out_ref.dtype)
        count = ref.shape[0] // size
        for j, block in enumerate(blocks[first:first + count]):
            start = pl.multiple_of(block * size, size)
            out_ref[pl.ds(start, size), :] = value[j * size:(j + 1) * size]
        first += count


def ratio_kernel(*refs, parts, z_count, slots, size):
    inv_refs, val_refs = refs[:parts], refs[parts:-3]
    slot_ref, rows_ref, ratio_ref = refs[-3:]
    val = jnp.concatenate([ref[...] for ref in val_refs], axis=1)
    inverse_times(z_count, inv_refs, val, ratio_ref, size)
    ratio = ratio_ref[...]
    slot = slot_ref[...]
    blocks = owners(z_count)
    for j in range(0, len(blocks), 2):
        ids = lax.broadcasted_iota(jnp.int32, (slots, slot.shape[1]), 0)
        pick = jnp.concatenate([(ids + block * slots == slot).astype(F32) for block in blocks[j:j + 2]], axis=0)
        rows_ref[j * slots:(j + 2) * slots, :] = mm(pick.astype(BF16), ratio).astype(BF16)


def coupled(rows_ref, pieces):
    total = None
    for first, ref in pieces:
        term = mm_tn(rows_ref[first:first + ref.shape[0], :], ref[...])
        total = term if total is None else total + term
    return total


def scale_kernel(energy_ref, weight_ref, scale_ref):
    line = lax.broadcasted_iota(jnp.int32, scale_ref.shape, 0)
    scale_ref[...] = jnp.where(line == 0, energy_ref[0], weight_ref[0])


def finish_kernel(scale_ref, near_own_ref, far_own_ref, near_other_ref, far_other_ref, rows_ref,
                  val_a, val_b, lap_a, lap_b, *refs, z_count, size):
    inv_refs, out_ref = refs[:-1], refs[-1]
    half = rows_ref.shape[0] // 2
    near = near_own_ref.shape[0]
    total = coupled(rows_ref, [
        (0, near_own_ref), (near, far_own_ref), (half, near_other_ref), (half + near, far_other_ref)
    ])
    val = jnp.concatenate([val_a[...], val_b[...]], axis=1).astype(F32)
    lap = jnp.concatenate([lap_a[...], lap_b[...]], axis=1).astype(F32)
    energy, weight = scale_ref[0:1, 0:1], scale_ref[1:2, 0:1]
    mixed = (weight * (energy * val - 0.5 * (lap - total))).astype(BF16)
    inverse_times(z_count, inv_refs, mixed, out_ref, size)


VMEM = pl.BlockSpec(memory_space=pltpu.VMEM)
SMEM = pl.BlockSpec(memory_space=pltpu.SMEM)
HBM = pl.BlockSpec(memory_space=pltpu.HBM)


def ring_swap(piece):
    return lax.ppermute(piece, "xh", [(0, 1), (1, 0)])


def ring_pass(piece, shift):
    count = lax.axis_size("z")
    return lax.ppermute(piece, "z", [(i, (i + shift) % count) for i in range(count)])


def core_swap(piece):
    return lax.ppermute(piece, "core", [(0, 1), (1, 0)])


def gradient(coefficients, inverse, cell_index, fraction, energies, weights, occupied):
    cells, width = coefficients.shape
    _, rows, electrons = inverse.shape
    z_count = lax.axis_size("z")
    shards = 2 * z_count * 2
    slots = 3 * electrons // (2 * shards)

    along_z = (2, 1, -1)
    out = lambda *shape_dtype: jax.ShapeDtypeStruct(*shape_dtype)
    halves = 2
    part = electrons // halves

    def params(mib):
        return pltpu.CompilerParams(vmem_limit_bytes=mib * 1024 * 1024)

    def cost(products):
        return pl.CostEstimate(flops=2 * products, bytes_accessed=2 * cells * width, transcendentals=0)

    def evaluate(h):
        return pl.pallas_call(
            functools.partial(eval_kernel, first=h * part),
            out_shape=[out((width, part), BF16)] * 2,
            in_specs=[VMEM] * 3,
            out_specs=[VMEM] * 2,
            scratch_shapes=[pltpu.VMEM((cells, TILE), BF16)] * 4,
            compiler_params=params(32),
            cost_estimate=cost(2 * part * cells * width),
            name="evaluate",
        )(turned, cell_index, fraction)

    cell_index, fraction = jnp.transpose(cell_index, (1, 0, 2)), jnp.transpose(fraction, (1, 0, 2))
    mine = inverse.reshape(rows, electrons)

    inv_pieces = [mine]
    for shift in along_z:
        inv_pieces.append(ring_pass(mine, shift))
    inv_plane = jnp.concatenate(inv_pieces, axis=0)
    inv_far = ring_swap(inv_plane)
    inv_plane_other = core_swap(inv_plane)
    inv_far_other = core_swap(inv_far)
    inv_all = [inv_plane, inv_far, inv_plane_other, inv_far_other]

    turned = pl.pallas_call(
        turn_kernel,
        out_shape=out((width, cells), BF16),
        in_specs=[HBM],
        out_specs=VMEM,
        scratch_shapes=[pltpu.VMEM((cells, width), BF16), pltpu.SemaphoreType.DMA((8,))],
        compiler_params=params(50),
        cost_estimate=cost(cells * width * 64),
        name="turn",
    )(coefficients)
    lapt_mine, slot = pl.pallas_call(
        functools.partial(early_kernel, shards=shards),
        out_shape=[out((slots, electrons), BF16), out((1, electrons), jnp.int32)],
        in_specs=[VMEM] * 4,
        out_specs=[VMEM] * 2,
        scratch_shapes=[pltpu.VMEM((cells, TILE), BF16)] * 2,
        compiler_params=params(32),
        cost_estimate=cost(slots * cells * electrons),
        name="early",
    )(turned, cell_index, fraction, occupied.reshape(1, electrons))
    val_a, lap_a = evaluate(0)
    val_b, lap_b = evaluate(1)

    lapt_far = ring_swap(lapt_mine)
    near, far = [lapt_mine], []
    for shift in along_z:
        near.append(ring_pass(lapt_mine, shift))
    near.append(lapt_far)
    for shift in along_z:
        far.append(ring_pass(lapt_far, shift))
    near = jnp.concatenate(near, axis=0)
    far = jnp.concatenate(far, axis=0)
    near_other = core_swap(near)
    far_other = core_swap(far)
    total = shards * slots

    ratio_rows = pl.pallas_call(
        functools.partial(ratio_kernel, parts=len(inv_all), z_count=z_count, slots=slots, size=rows),
        out_shape=out((total, width), BF16),
        in_specs=[VMEM] * (len(inv_all) + 3),
        out_specs=VMEM,
        scratch_shapes=[pltpu.VMEM((electrons, width), BF16)],
        compiler_params=params(24),
        cost_estimate=cost(3 * electrons * electrons * width),
        name="ratio",
    )(*inv_all, val_a, val_b, slot)

    scale = pl.pallas_call(
        scale_kernel,
        out_shape=out((2, 128), F32),
        in_specs=[SMEM] * 2,
        out_specs=VMEM,
        compiler_params=params(1),
        name="scale",
    )(energies, weights)
    partial = pl.pallas_call(
        functools.partial(finish_kernel, z_count=z_count, size=rows),
        out_shape=out((electrons, width), BF16),
        in_specs=[VMEM] * (10 + len(inv_all)),
        out_specs=VMEM,
        compiler_params=params(24),
        cost_estimate=cost(3 * electrons * electrons * width),
        name="finish",
    )(scale, near, far, near_other, far_other, ratio_rows, val_a, val_b, lap_a, lap_b, *inv_all)

    walkers = ("y", "xl")
    count = lax.axis_size(walkers)
    blocks = lax.all_to_all(partial.reshape(count, electrons // count, width), walkers, 0, 0, tiled=True)
    return jnp.sum(blocks.astype(F32), axis=0)


def solution(mesh):
    fine = Mesh(mesh.devices.reshape(4, 2, 2, 4, 2), ("y", "xl", "xh", "z", "core"))
    walk, orb = ("y", "xl"), ("xh", "z", "core")
    in_specs = (
        P(None, orb),
        P(walk, orb, None),
        P(walk, None, None),
        P(walk, None, None),
        P(walk),
        P(walk),
        P(),
    )
    return jax.shard_map(gradient, mesh=fine, in_specs=in_specs, out_specs=P(walk, orb), check_vma=False)
```

```python
import functools

import jax
import jax.numpy as jnp
from jax import lax
from jax.experimental import pallas as pl
from jax.experimental.pallas import tpu as pltpu
from jax.sharding import Mesh
from jax.sharding import PartitionSpec as P


GRID = 16
PLANE = GRID * GRID
TILE = 256
BF16 = jnp.bfloat16
F32 = jnp.float32


def mm(left, right):
    return jnp.dot(left, right, preferred_element_type=F32)


def mm_nt(left, right):
    return lax.dot_general(left, right, (((1,), (1,)), ((), ())), preferred_element_type=F32)


def mm_tn(left, right):
    return lax.dot_general(left, right, (((0,), (0,)), ((), ())), preferred_element_type=F32)


def dense_rows(cell, frac):
    remain = 1.0 - frac
    square = frac * frac
    cubed = square * frac
    sixth = 1.0 / 6.0
    values = [
        remain * remain * remain * sixth,
        (3.0 * cubed - 6.0 * square + 4.0) * sixth,
        (-3.0 * cubed + 3.0 * square + 3.0 * frac + 1.0) * sixth,
        cubed * sixth,
    ]
    curves = [remain, 3.0 * frac - 2.0, 1.0 - 3.0 * frac, frac]
    line = lax.broadcasted_iota(jnp.int32, (GRID, cell.shape[1]), 0)
    tap = (line - cell + (GRID + 1)) & (GRID - 1)
    value = jnp.zeros((GRID, cell.shape[1]), F32)
    curve = jnp.zeros((GRID, cell.shape[1]), F32)
    for a in range(4):
        value = jnp.where(tap == a, values[a], value)
        curve = jnp.where(tap == a, curves[a], curve)
    return value, curve


def slot_tables(me, occ, shards, width, slots):
    owner = lax.broadcasted_iota(jnp.int32, (shards, occ.shape[1]), 0) == lax.div(occ, width)
    count = owner.astype(jnp.int32)
    lane = lax.broadcasted_iota(jnp.int32, count.shape, 1)
    step = 1
    while step < occ.shape[1]:
        count = count + jnp.where(lane >= step, pltpu.roll(count, step, 1), 0)
        step *= 2
    rank = jnp.sum(jnp.where(owner, count - 1, 0), axis=0, keepdims=True)
    slot = lax.div(occ, width) * slots + rank
    placed = lax.broadcasted_iota(jnp.int32, (slots, occ.shape[1]), 0) == slot - me * slots
    column = lax.broadcasted_iota(jnp.int32, (width, occ.shape[1]), 0) == occ - me * width
    picker = mm_nt(placed.astype(F32).astype(BF16), column.astype(F32).astype(BF16)).astype(BF16)
    return slot, picker


def expand(rows, weights):
    return jnp.concatenate([rows[g:g + 1, :] * weights for g in range(GRID)], axis=0)


def first_kernel(flag_ref):
    flag_ref[...] = jnp.zeros(flag_ref.shape, F32)


def weight_tables(cell_ref, frac_ref, here):
    tables = [dense_rows(cell_ref[k, :, here], frac_ref[k, :, here]) for k in range(3)]
    (vx, cx), (vy, cy), (vz, cz) = tables
    return vx, cx, expand(vy, vz), expand(cy, vz) + expand(vy, cz)


def build_laplacian(tables, w_ref):
    vx, cx, value, curve = tables
    for g in range(GRID):
        w_ref[g * PLANE:(g + 1) * PLANE, :] = (cx[g:g + 1, :] * value + vx[g:g + 1, :] * curve).astype(BF16)


def build_value(tables, w_ref):
    vx, _, value, _ = tables
    for g in range(GRID):
        w_ref[g * PLANE:(g + 1) * PLANE, :] = (vx[g:g + 1, :] * value).astype(BF16)


def early_kernel(flag_ref, coef_ref, cell_ref, frac_ref, occ_ref, lapt_ref, slot_ref, *w_refs, shards):
    slots, electrons = lapt_ref.shape
    plane, along, core = place(shards // 4)
    me = (plane * (shards // 4) + along[0]) * 2 + core
    slot, picker = slot_tables(me, occ_ref[...], shards, coef_ref.shape[1], slots)
    slot_ref[...] = slot
    chosen = mm_nt(picker, coef_ref[...]).astype(BF16)

    def build(t):
        vx, cx, value, curve = weight_tables(cell_ref, frac_ref, slice(t * TILE, (t + 1) * TILE))
        value = value.astype(BF16).reshape(GRID, GRID, TILE)
        curve = curve.astype(BF16).reshape(GRID, GRID, TILE)
        for g in range(GRID):
            x_value = jnp.broadcast_to(vx[g:g + 1, :], (GRID, TILE)).astype(BF16)[None]
            x_curve = jnp.broadcast_to(cx[g:g + 1, :], (GRID, TILE)).astype(BF16)[None]
            w_refs[t % 2][g * PLANE:(g + 1) * PLANE, :] = (x_curve * value + x_value * curve).reshape(PLANE, TILE)

    build(0)
    for t in range(electrons // TILE):
        if (t + 1) * TILE < electrons:
            build(t + 1)
        lapt_ref[:, t * TILE:(t + 1) * TILE] = mm(chosen, w_refs[t % 2][...]).astype(BF16)


def eval_kernel(coef_ref, cell_ref, frac_ref, val_ref, lap_ref, *w_refs, first):
    electrons = val_ref.shape[1]
    turned_ref = coef_ref
    if first == 0:
        turned_ref, *w_refs = w_refs
        for g in range(GRID):
            turned_ref[:, g * PLANE:(g + 1) * PLANE] = jnp.transpose(coef_ref[g * PLANE:(g + 1) * PLANE, :])

    def build(t):
        tables = weight_tables(cell_ref, frac_ref, slice(first + t * TILE, first + (t + 1) * TILE))
        build_value(tables, w_refs[2 * (t % 2)])
        build_laplacian(tables, w_refs[2 * (t % 2) + 1])

    build(0)
    for t in range(electrons // TILE):
        if (t + 1) * TILE < electrons:
            build(t + 1)
        here = slice(t * TILE, (t + 1) * TILE)
        val_ref[:, here] = mm(turned_ref[...], w_refs[2 * (t % 2)][...]).astype(BF16)
        lap_ref[:, here] = mm(turned_ref[...], w_refs[2 * (t % 2) + 1][...]).astype(BF16)


def place(z_count):
    core, z, plane = lax.axis_index("core"), lax.axis_index("z"), lax.axis_index("xh")
    return plane, [lax.rem(z + dz, z_count) for dz in (0, 2, z_count - 1, 1)], core


def owners(z_count):
    plane, along, core = place(z_count)
    return [(p * z_count + z) * 2 + c for c in (core, 1 - core) for p in (plane, 1 - plane) for z in along]


def inverse_times(z_count, inv_refs, right, out_ref, size):
    blocks = owners(z_count)
    first = 0
    for ref in inv_refs:
        value = mm_nt(ref[...], right).astype(out_ref.dtype)
        count = ref.shape[0] // size
        for j, block in enumerate(blocks[first:first + count]):
            start = pl.multiple_of(block * size, size)
            out_ref[pl.ds(start, size), :] = value[j * size:(j + 1) * size]
        first += count


def ratio_kernel(*refs, parts, z_count, slots, size):
    inv_refs, val_refs = refs[:parts], refs[parts:-3]
    slot_ref, rows_ref, ratio_ref = refs[-3:]
    val = jnp.concatenate([ref[...] for ref in val_refs], axis=1)
    inverse_times(z_count, inv_refs, val, ratio_ref, size)
    ratio = ratio_ref[...]
    slot = slot_ref[...]
    blocks = owners(z_count)
    for j in range(0, len(blocks), 2):
        ids = lax.broadcasted_iota(jnp.int32, (slots, slot.shape[1]), 0)
        pick = jnp.concatenate([(ids + block * slots == slot).astype(F32) for block in blocks[j:j + 2]], axis=0)
        rows_ref[j * slots:(j + 2) * slots, :] = mm(pick.astype(BF16), ratio).astype(BF16)


def coupled(rows_ref, pieces):
    total = None
    for first, ref in pieces:
        term = mm_tn(rows_ref[first:first + ref.shape[0], :], ref[...])
        total = term if total is None else total + term
    return total


def scale_kernel(energy_ref, weight_ref, scale_ref):
    line = lax.broadcasted_iota(jnp.int32, scale_ref.shape, 0)
    scale_ref[...] = jnp.where(line == 0, energy_ref[0], weight_ref[0])


def finish_kernel(scale_ref, near_own_ref, far_own_ref, near_other_ref, far_other_ref, rows_ref,
                  val_a, val_b, lap_a, lap_b, *refs, z_count, size):
    inv_refs, out_ref = refs[:-1], refs[-1]
    half = rows_ref.shape[0] // 2
    near = near_own_ref.shape[0]
    total = coupled(rows_ref, [
        (0, near_own_ref), (near, far_own_ref), (half, near_other_ref), (half + near, far_other_ref)
    ])
    val = jnp.concatenate([val_a[...], val_b[...]], axis=1).astype(F32)
    lap = jnp.concatenate([lap_a[...], lap_b[...]], axis=1).astype(F32)
    energy, weight = scale_ref[0:1, 0:1], scale_ref[1:2, 0:1]
    mixed = (weight * (energy * val - 0.5 * (lap - total))).astype(BF16)
    inverse_times(z_count, inv_refs, mixed, out_ref, size)


VMEM = pl.BlockSpec(memory_space=pltpu.VMEM)
SMEM = pl.BlockSpec(memory_space=pltpu.SMEM)


def ring_swap(piece):
    return lax.ppermute(piece, "xh", [(0, 1), (1, 0)])


def ring_pass(piece, shift):
    count = lax.axis_size("z")
    return lax.ppermute(piece, "z", [(i, (i + shift) % count) for i in range(count)])


def core_swap(piece):
    return lax.ppermute(piece, "core", [(0, 1), (1, 0)])


def gradient(coefficients, inverse, cell_index, fraction, energies, weights, occupied):
    cells, width = coefficients.shape
    _, rows, electrons = inverse.shape
    z_count = lax.axis_size("z")
    shards = 2 * z_count * 2
    slots = 3 * electrons // (2 * shards)

    along_z = (2, 1, -1)
    out = lambda *shape_dtype: jax.ShapeDtypeStruct(*shape_dtype)
    halves = 2
    part = electrons // halves

    def params(mib):
        return pltpu.CompilerParams(vmem_limit_bytes=mib * 1024 * 1024)

    def cost(products):
        return pl.CostEstimate(flops=2 * products, bytes_accessed=2 * cells * width, transcendentals=0)

    def evaluate(h, coef):
        results = [out((width, part), BF16)] * 2 + ([out((width, cells), BF16)] if h == 0 else [])
        return pl.pallas_call(
            functools.partial(eval_kernel, first=h * part),
            out_shape=results,
            in_specs=[VMEM] * 3,
            out_specs=[VMEM] * len(results),
            scratch_shapes=[pltpu.VMEM((cells, TILE), BF16)] * 4,
            compiler_params=params(32),
            cost_estimate=cost(2 * part * cells * width),
            name="evaluate",
        )(coef, cell_index, fraction)

    cell_index, fraction = jnp.transpose(cell_index, (1, 0, 2)), jnp.transpose(fraction, (1, 0, 2))
    mine = inverse.reshape(rows, electrons)

    inv_pieces = [mine]
    for shift in along_z:
        inv_pieces.append(ring_pass(mine, shift))
    inv_plane = jnp.concatenate(inv_pieces, axis=0)
    inv_far = ring_swap(inv_plane)
    inv_plane_other = core_swap(inv_plane)
    inv_far_other = core_swap(inv_far)
    inv_all = [inv_plane, inv_far, inv_plane_other, inv_far_other]

    flag = pl.pallas_call(
        first_kernel,
        out_shape=out((8, 128), F32),
        out_specs=VMEM,
        compiler_params=params(1),
        cost_estimate=pl.CostEstimate(flops=10**10, bytes_accessed=10**8, transcendentals=0),
        name="first",
    )()
    lapt_mine, slot = pl.pallas_call(
        functools.partial(early_kernel, shards=shards),
        out_shape=[out((slots, electrons), BF16), out((1, electrons), jnp.int32)],
        in_specs=[VMEM] * 5,
        out_specs=[VMEM] * 2,
        scratch_shapes=[pltpu.VMEM((cells, TILE), BF16)] * 2,
        compiler_params=params(32),
        cost_estimate=cost(slots * cells * electrons),
        name="early",
    )(flag, coefficients, cell_index, fraction, occupied.reshape(1, electrons))
    val_a, lap_a, turned = evaluate(0, coefficients)
    val_b, lap_b = evaluate(1, turned)

    lapt_far = ring_swap(lapt_mine)
    near, far = [lapt_mine], []
    for shift in along_z:
        near.append(ring_pass(lapt_mine, shift))
    near.append(lapt_far)
    for shift in along_z:
        far.append(ring_pass(lapt_far, shift))
    near = jnp.concatenate(near, axis=0)
    far = jnp.concatenate(far, axis=0)
    near_other = core_swap(near)
    far_other = core_swap(far)
    total = shards * slots

    ratio_rows = pl.pallas_call(
        functools.partial(ratio_kernel, parts=len(inv_all), z_count=z_count, slots=slots, size=rows),
        out_shape=out((total, width), BF16),
        in_specs=[VMEM] * (len(inv_all) + 3),
        out_specs=VMEM,
        scratch_shapes=[pltpu.VMEM((electrons, width), BF16)],
        compiler_params=params(24),
        cost_estimate=cost(3 * electrons * electrons * width),
        name="ratio",
    )(*inv_all, val_a, val_b, slot)

    scale = pl.pallas_call(
        scale_kernel,
        out_shape=out((2, 128), F32),
        in_specs=[SMEM] * 2,
        out_specs=VMEM,
        compiler_params=params(1),
        name="scale",
    )(energies, weights)
    partial = pl.pallas_call(
        functools.partial(finish_kernel, z_count=z_count, size=rows),
        out_shape=out((electrons, width), BF16),
        in_specs=[VMEM] * (10 + len(inv_all)),
        out_specs=VMEM,
        compiler_params=params(24),
        cost_estimate=cost(3 * electrons * electrons * width),
        name="finish",
    )(scale, near, far, near_other, far_other, ratio_rows, val_a, val_b, lap_a, lap_b, *inv_all)

    walkers = ("y", "xl")
    count = lax.axis_size(walkers)
    blocks = lax.all_to_all(partial.reshape(count, electrons // count, width), walkers, 0, 0, tiled=True)
    return jnp.sum(blocks.astype(F32), axis=0)


def solution(mesh):
    fine = Mesh(mesh.devices.reshape(4, 2, 2, 4, 2), ("y", "xl", "xh", "z", "core"))
    walk, orb = ("y", "xl"), ("xh", "z", "core")
    in_specs = (
        P(None, orb),
        P(walk, orb, None),
        P(walk, None, None),
        P(walk, None, None),
        P(walk),
        P(walk),
        P(),
    )
    return jax.shard_map(gradient, mesh=fine, in_specs=in_specs, out_specs=P(walk, orb), check_vma=False)
```

```python
import functools

import jax
import jax.numpy as jnp
from jax import lax
from jax.experimental import pallas as pl
from jax.experimental.pallas import tpu as pltpu
from jax.sharding import Mesh
from jax.sharding import PartitionSpec as P


GRID = 16
PLANE = GRID * GRID
TILE = 256
BF16 = jnp.bfloat16
F32 = jnp.float32


def mm(left, right):
    return jnp.dot(left, right, preferred_element_type=F32)


def mm_nt(left, right):
    return lax.dot_general(left, right, (((1,), (1,)), ((), ())), preferred_element_type=F32)


def mm_tn(left, right):
    return lax.dot_general(left, right, (((0,), (0,)), ((), ())), preferred_element_type=F32)


def dense_rows(cell, frac):
    remain = 1.0 - frac
    square = frac * frac
    cubed = square * frac
    sixth = 1.0 / 6.0
    values = [
        remain * remain * remain * sixth,
        (3.0 * cubed - 6.0 * square + 4.0) * sixth,
        (-3.0 * cubed + 3.0 * square + 3.0 * frac + 1.0) * sixth,
        cubed * sixth,
    ]
    curves = [remain, 3.0 * frac - 2.0, 1.0 - 3.0 * frac, frac]
    line = lax.broadcasted_iota(jnp.int32, (GRID, cell.shape[1]), 0)
    tap = (line - cell + (GRID + 1)) & (GRID - 1)
    value = jnp.zeros((GRID, cell.shape[1]), F32)
    curve = jnp.zeros((GRID, cell.shape[1]), F32)
    for a in range(4):
        value = jnp.where(tap == a, values[a], value)
        curve = jnp.where(tap == a, curves[a], curve)
    return value, curve


def slot_tables(me, occ, shards, width, slots):
    owner = lax.broadcasted_iota(jnp.int32, (shards, occ.shape[1]), 0) == lax.div(occ, width)
    count = owner.astype(jnp.int32)
    lane = lax.broadcasted_iota(jnp.int32, count.shape, 1)
    step = 1
    while step < occ.shape[1]:
        count = count + jnp.where(lane >= step, pltpu.roll(count, step, 1), 0)
        step *= 2
    rank = jnp.sum(jnp.where(owner, count - 1, 0), axis=0, keepdims=True)
    slot = lax.div(occ, width) * slots + rank
    placed = lax.broadcasted_iota(jnp.int32, (slots, occ.shape[1]), 0) == slot - me * slots
    column = lax.broadcasted_iota(jnp.int32, (width, occ.shape[1]), 0) == occ - me * width
    picker = mm_nt(placed.astype(F32).astype(BF16), column.astype(F32).astype(BF16)).astype(BF16)
    return slot, picker


def expand(rows, weights):
    return jnp.concatenate([rows[g:g + 1, :] * weights for g in range(GRID)], axis=0)


def first_kernel(flag_ref):
    flag_ref[...] = jnp.zeros(flag_ref.shape, F32)


def weight_tables(cell_ref, frac_ref, here):
    tables = [dense_rows(cell_ref[k, :, here], frac_ref[k, :, here]) for k in range(3)]
    (vx, cx), (vy, cy), (vz, cz) = tables
    return vx, cx, expand(vy, vz), expand(cy, vz) + expand(vy, cz)


def build_laplacian(tables, w_ref):
    vx, cx, value, curve = tables
    for g in range(GRID):
        w_ref[g * PLANE:(g + 1) * PLANE, :] = (cx[g:g + 1, :] * value + vx[g:g + 1, :] * curve).astype(BF16)


def build_value(tables, w_ref):
    vx, _, value, _ = tables
    for g in range(GRID):
        w_ref[g * PLANE:(g + 1) * PLANE, :] = (vx[g:g + 1, :] * value).astype(BF16)


def early_kernel(flag_ref, coef_ref, cell_ref, frac_ref, occ_ref, lapt_ref, slot_ref, *w_refs, shards):
    slots, electrons = lapt_ref.shape
    plane, along, core = place(shards // 4)
    me = (plane * (shards // 4) + along[0]) * 2 + core
    slot, picker = slot_tables(me, occ_ref[...], shards, coef_ref.shape[1], slots)
    slot_ref[...] = slot
    chosen = mm_nt(picker, coef_ref[...]).astype(BF16)

    def build(start, w_ref):
        vx, cx, value, curve = weight_tables(cell_ref, frac_ref, pl.ds(start, TILE))
        value = value.astype(BF16).reshape(GRID, GRID, TILE)
        curve = curve.astype(BF16).reshape(GRID, GRID, TILE)
        for g in range(GRID):
            x_value = jnp.broadcast_to(vx[g:g + 1, :], (GRID, TILE)).astype(BF16)[None]
            x_curve = jnp.broadcast_to(cx[g:g + 1, :], (GRID, TILE)).astype(BF16)[None]
            w_ref[g * PLANE:(g + 1) * PLANE, :] = (x_curve * value + x_value * curve).reshape(PLANE, TILE)

    chosen_ref, *w_refs = w_refs
    chosen_ref[...] = chosen

    def step(i, carry):
        starts = [pl.multiple_of((i * len(w_refs) + k) * TILE, TILE) for k in range(len(w_refs))]
        for start, w_ref in zip(starts, w_refs):
            build(start, w_ref)
        for start, w_ref in zip(starts, w_refs):
            lapt_ref[:, pl.ds(start, TILE)] = mm(chosen_ref[...], w_ref[...]).astype(BF16)
        return carry

    lax.fori_loop(0, electrons // (TILE * len(w_refs)), step, 0)


def eval_kernel(coef_ref, cell_ref, frac_ref, val_ref, lap_ref, *w_refs, first):
    electrons = val_ref.shape[1]
    turned_ref = coef_ref
    if first == 0:
        turned_ref, *w_refs = w_refs
        for g in range(GRID):
            turned_ref[:, g * PLANE:(g + 1) * PLANE] = jnp.transpose(coef_ref[g * PLANE:(g + 1) * PLANE, :])

    def build(t):
        tables = weight_tables(cell_ref, frac_ref, slice(first + t * TILE, first + (t + 1) * TILE))
        build_value(tables, w_refs[2 * (t % 2)])
        build_laplacian(tables, w_refs[2 * (t % 2) + 1])

    build(0)
    for t in range(electrons // TILE):
        if (t + 1) * TILE < electrons:
            build(t + 1)
        here = slice(t * TILE, (t + 1) * TILE)
        val_ref[:, here] = mm(turned_ref[...], w_refs[2 * (t % 2)][...]).astype(BF16)
        lap_ref[:, here] = mm(turned_ref[...], w_refs[2 * (t % 2) + 1][...]).astype(BF16)


def place(z_count):
    core, z, plane = lax.axis_index("core"), lax.axis_index("z"), lax.axis_index("xh")
    return plane, [lax.rem(z + dz, z_count) for dz in (0, 2, z_count - 1, 1)], core


def owners(z_count):
    plane, along, core = place(z_count)
    return [(p * z_count + z) * 2 + c for c in (core, 1 - core) for p in (plane, 1 - plane) for z in along]


def inverse_times(z_count, inv_refs, right, out_ref, size):
    blocks = owners(z_count)
    first = 0
    for ref in inv_refs:
        value = mm_nt(ref[...], right).astype(out_ref.dtype)
        count = ref.shape[0] // size
        for j, block in enumerate(blocks[first:first + count]):
            start = pl.multiple_of(block * size, size)
            out_ref[pl.ds(start, size), :] = value[j * size:(j + 1) * size]
        first += count


def ratio_kernel(*refs, parts, z_count, slots, size):
    inv_refs, val_refs = refs[:parts], refs[parts:-3]
    slot_ref, rows_ref, ratio_ref = refs[-3:]
    val = jnp.concatenate([ref[...] for ref in val_refs], axis=1)
    inverse_times(z_count, inv_refs, val, ratio_ref, size)
    ratio = ratio_ref[...]
    slot = slot_ref[...]
    blocks = owners(z_count)
    for j in range(0, len(blocks), 2):
        ids = lax.broadcasted_iota(jnp.int32, (slots, slot.shape[1]), 0)
        pick = jnp.concatenate([(ids + block * slots == slot).astype(F32) for block in blocks[j:j + 2]], axis=0)
        rows_ref[j * slots:(j + 2) * slots, :] = mm(pick.astype(BF16), ratio).astype(BF16)


def coupled(rows_ref, pieces):
    total = None
    for first, ref in pieces:
        term = mm_tn(rows_ref[first:first + ref.shape[0], :], ref[...])
        total = term if total is None else total + term
    return total


def scale_kernel(energy_ref, weight_ref, scale_ref):
    line = lax.broadcasted_iota(jnp.int32, scale_ref.shape, 0)
    scale_ref[...] = jnp.where(line == 0, energy_ref[0], weight_ref[0])


def finish_kernel(scale_ref, near_own_ref, far_own_ref, near_other_ref, far_other_ref, rows_ref,
                  val_a, val_b, lap_a, lap_b, *refs, z_count, size):
    inv_refs, out_ref = refs[:-1], refs[-1]
    half = rows_ref.shape[0] // 2
    near = near_own_ref.shape[0]
    total = coupled(rows_ref, [
        (0, near_own_ref), (near, far_own_ref), (half, near_other_ref), (half + near, far_other_ref)
    ])
    val = jnp.concatenate([val_a[...], val_b[...]], axis=1).astype(F32)
    lap = jnp.concatenate([lap_a[...], lap_b[...]], axis=1).astype(F32)
    energy, weight = scale_ref[0:1, 0:1], scale_ref[1:2, 0:1]
    mixed = (weight * (energy * val - 0.5 * (lap - total))).astype(BF16)
    inverse_times(z_count, inv_refs, mixed, out_ref, size)


VMEM = pl.BlockSpec(memory_space=pltpu.VMEM)
SMEM = pl.BlockSpec(memory_space=pltpu.SMEM)


def ring_swap(piece):
    return lax.ppermute(piece, "xh", [(0, 1), (1, 0)])


def ring_pass(piece, shift):
    count = lax.axis_size("z")
    return lax.ppermute(piece, "z", [(i, (i + shift) % count) for i in range(count)])


def core_swap(piece):
    return lax.ppermute(piece, "core", [(0, 1), (1, 0)])


def gradient(coefficients, inverse, cell_index, fraction, energies, weights, occupied):
    cells, width = coefficients.shape
    _, rows, electrons = inverse.shape
    z_count = lax.axis_size("z")
    shards = 2 * z_count * 2
    slots = 3 * electrons // (2 * shards)

    along_z = (2, 1, -1)
    out = lambda *shape_dtype: jax.ShapeDtypeStruct(*shape_dtype)
    halves = 2
    part = electrons // halves

    def params(mib):
        return pltpu.CompilerParams(vmem_limit_bytes=mib * 1024 * 1024)

    def cost(products):
        return pl.CostEstimate(flops=2 * products, bytes_accessed=2 * cells * width, transcendentals=0)

    def evaluate(h, coef):
        results = [out((width, part), BF16)] * 2 + ([out((width, cells), BF16)] if h == 0 else [])
        return pl.pallas_call(
            functools.partial(eval_kernel, first=h * part),
            out_shape=results,
            in_specs=[VMEM] * 3,
            out_specs=[VMEM] * len(results),
            scratch_shapes=[pltpu.VMEM((cells, TILE), BF16)] * 4,
            compiler_params=params(32),
            cost_estimate=cost(2 * part * cells * width),
            name="evaluate",
        )(coef, cell_index, fraction)

    cell_index, fraction = jnp.transpose(cell_index, (1, 0, 2)), jnp.transpose(fraction, (1, 0, 2))
    mine = inverse.reshape(rows, electrons)

    inv_pieces = [mine]
    for shift in along_z:
        inv_pieces.append(ring_pass(mine, shift))
    inv_plane = jnp.concatenate(inv_pieces, axis=0)
    inv_far = ring_swap(inv_plane)
    inv_plane_other = core_swap(inv_plane)
    inv_far_other = core_swap(inv_far)
    inv_all = [inv_plane, inv_far, inv_plane_other, inv_far_other]

    flag = pl.pallas_call(
        first_kernel,
        out_shape=out((8, 128), F32),
        out_specs=VMEM,
        compiler_params=params(1),
        cost_estimate=pl.CostEstimate(flops=10**10, bytes_accessed=10**8, transcendentals=0),
        name="first",
    )()
    lapt_mine, slot = pl.pallas_call(
        functools.partial(early_kernel, shards=shards),
        out_shape=[out((slots, electrons), BF16), out((1, electrons), jnp.int32)],
        in_specs=[VMEM] * 5,
        out_specs=[VMEM] * 2,
        scratch_shapes=[pltpu.VMEM((slots, cells), BF16)] + [pltpu.VMEM((cells, TILE), BF16)] * 2,
        compiler_params=params(32),
        cost_estimate=cost(slots * cells * electrons),
        name="early",
    )(flag, coefficients, cell_index, fraction, occupied.reshape(1, electrons))
    val_a, lap_a, turned = evaluate(0, coefficients)
    val_b, lap_b = evaluate(1, turned)

    lapt_far = ring_swap(lapt_mine)
    near, far = [lapt_mine], []
    for shift in along_z:
        near.append(ring_pass(lapt_mine, shift))
    near.append(lapt_far)
    for shift in along_z:
        far.append(ring_pass(lapt_far, shift))
    near = jnp.concatenate(near, axis=0)
    far = jnp.concatenate(far, axis=0)
    near_other = core_swap(near)
    far_other = core_swap(far)
    total = shards * slots

    ratio_rows = pl.pallas_call(
        functools.partial(ratio_kernel, parts=len(inv_all), z_count=z_count, slots=slots, size=rows),
        out_shape=out((total, width), BF16),
        in_specs=[VMEM] * (len(inv_all) + 3),
        out_specs=VMEM,
        scratch_shapes=[pltpu.VMEM((electrons, width), BF16)],
        compiler_params=params(24),
        cost_estimate=cost(3 * electrons * electrons * width),
        name="ratio",
    )(*inv_all, val_a, val_b, slot)

    scale = pl.pallas_call(
        scale_kernel,
        out_shape=out((2, 128), F32),
        in_specs=[SMEM] * 2,
        out_specs=VMEM,
        compiler_params=params(1),
        name="scale",
    )(energies, weights)
    partial = pl.pallas_call(
        functools.partial(finish_kernel, z_count=z_count, size=rows),
        out_shape=out((electrons, width), BF16),
        in_specs=[VMEM] * (10 + len(inv_all)),
        out_specs=VMEM,
        compiler_params=params(24),
        cost_estimate=cost(3 * electrons * electrons * width),
        name="finish",
    )(scale, near, far, near_other, far_other, ratio_rows, val_a, val_b, lap_a, lap_b, *inv_all)

    walkers = ("y", "xl")
    count = lax.axis_size(walkers)
    blocks = lax.all_to_all(partial.reshape(count, electrons // count, width), walkers, 0, 0, tiled=True)
    return jnp.sum(blocks.astype(F32), axis=0)


def solution(mesh):
    fine = Mesh(mesh.devices.reshape(4, 2, 2, 4, 2), ("y", "xl", "xh", "z", "core"))
    walk, orb = ("y", "xl"), ("xh", "z", "core")
    in_specs = (
        P(None, orb),
        P(walk, orb, None),
        P(walk, None, None),
        P(walk, None, None),
        P(walk),
        P(walk),
        P(),
    )
    return jax.shard_map(gradient, mesh=fine, in_specs=in_specs, out_specs=P(walk, orb), check_vma=False)
```
